32 devices in a mesh: rows: 8 (over z, y), cols: 4 (over x, core).
Axes of the slice: x: 2, y: 2, z: 4, core: 2. Of those that a mesh axis runs over, the one named last changes fastest.
Arguments:
- factor_a: bfloat16 [16384, 48, 48], P('rows'), may hold values from -0.875 to 0.875
- factor_b: bfloat16 [16384, 48, 48], P('rows'), may hold values from -0.046875 to 0.046875
- next_factor: bfloat16 [16384, 48, 48], P(('rows', 'cols')), may hold values from -6 to 6
- sketch_leg: bfloat16 [48, 32], replicated, may hold values from -6 to 6
- sketch_rows: bfloat16 [16384, 32], P('rows', 'cols'), may hold values from -6 to 6
Outputs:
- basis: float32 [32, 16384, 48], P(None, ('rows', 'cols'))
- squeezed: float32 [32, 48], replicated
The draws below stay inside these ranges and needn't reach their ends.
All inputs are finite; a program needn't handle non-finite values.
Results may differ from the reference program's by a relative error of at most 0.0003.
Values sent between devices are 32-bit elements; how exact they have to be, the bound alone decides.
No kernel may reach another device: no remote copies, remote signals or barrier semaphores. Data moves between devices by JAX's collectives and lax.ppermute only.
A program may use at most 128 MiB of HBM per device.

```python
import jax
import jax.numpy as jnp
from jax import lax

D = 48
P_SIZE = 32
NS = 16384


def steps_of(key, dims, split, smallest, largest):
    def one(axis_at, shards_of):
        steps = jax.random.uniform(jax.random.fold_in(jax.random.fold_in(key, 6), axis_at), (shards_of,), jnp.float32, smallest / len(split), largest / len(split))
        return jnp.repeat(jnp.exp(steps), dims[axis_at] // shards_of).reshape((-1,) + (1,) * (len(dims) - axis_at - 1))

    loudness = one(*split[0])
    for cut in split[1:]:
        loudness = loudness * one(*cut)
    return loudness


def noise(own_key, dims, deviation, most, shards=(), dtype=jnp.bfloat16):
    factor_of = steps_of(own_key, dims, shards, -0.22, 0.18) if shards else 1.0
    result = jax.random.normal(own_key, dims, jnp.float32) * deviation * factor_of
    return jnp.minimum(jnp.maximum(result, -most), most).astype(dtype)


def setup_inputs(seed: int = 0) -> dict:
    key_list = jax.random.split(jax.random.key(seed), 6)
    return {
        "factor_a": noise(key_list[0], (NS, D, D), D ** -0.5, 0.875, ((0, 8),)),
        "factor_b": noise(key_list[1], (NS, D, D), NS ** -0.5, 0.046875, ((0, 8),)),
        "next_factor": noise(key_list[2], (NS, D, D), 1.0, 6.0, ((0, 32),)),
        "sketch_leg": noise(key_list[3], (D, P_SIZE), 1.0, 6.0),
        "sketch_rows": noise(key_list[4], (NS, P_SIZE), 1.0, 6.0, ((0, 8), (1, 4))),
    }


def reference(factor_a, factor_b, next_factor, sketch_leg, sketch_rows):
    high = lax.Precision.HIGHEST
    far = jnp.einsum('sp,syk->pyk', sketch_rows.astype(jnp.float32), factor_b.astype(jnp.float32), precision=high)
    near = jnp.einsum('sxk,xp->psk', factor_a.astype(jnp.float32), sketch_leg.astype(jnp.float32), precision=high)
    sketch = jnp.einsum('psk,pyk->psy', near, far, precision=high)
    count = NS * D
    flat = sketch.reshape(P_SIZE, count)
    gram = jnp.dot(flat, flat.T, precision=high) / count
    lower = jnp.linalg.cholesky(gram)
    basis = jax.scipy.linalg.solve_triangular(lower, flat, lower=True)
    squeezed = jnp.dot(basis, next_factor.reshape(count, D).astype(jnp.float32), precision=high) / jnp.sqrt(jnp.float32(count))
    return (basis.reshape(P_SIZE, NS, D), squeezed)
```

```python
import jax
import jax.numpy as jnp
from jax import lax
from jax.sharding import PartitionSpec as P

BOTH = ("rows", "cols")


def gather_all(value):
    parts = lax.axis_size("rows") * lax.axis_size("cols")
    return lax.all_to_all(jnp.broadcast_to(value[None], (parts,) + value.shape), BOTH, 0, 0)


def per_device(factor_a, factor_b, next_factor, sketch_leg, sketch_rows):
    high = lax.Precision.HIGHEST
    f32 = jnp.float32
    rows, cols = lax.axis_size("rows"), lax.axis_size("cols")
    local_rows, width, bond = factor_a.shape
    quarter = local_rows // cols
    start = lax.axis_index("cols") * quarter
    count = local_rows * rows * width
    a = jnp.transpose(factor_a, (1, 2, 0))
    b = jnp.transpose(factor_b, (1, 2, 0))
    nxt = jnp.transpose(next_factor, (1, 2, 0))
    far_part = jnp.einsum("sp,yks->pyk", sketch_rows, b, preferred_element_type=f32)
    own = far_part.shape[0]
    each = -(-width // rows)
    far_part = jnp.pad(far_part, ((0, 0), (0, each * rows - width), (0, 0)))
    pieces = jnp.transpose(far_part.reshape(own, rows, each, bond), (1, 0, 2, 3))
    piece = jnp.sum(lax.all_to_all(pieces.reshape(rows, -1, 128), "rows", 0, 0), axis=0)
    far = gather_all(piece).reshape(rows, cols * own, each, bond)
    far = jnp.transpose(far, (1, 0, 2, 3)).reshape(cols * own, rows * each, bond)[:, :width]
    own_a = lax.dynamic_slice_in_dim(a, start, quarter, 2)
    near = jnp.einsum("xks,xp->pks", own_a, sketch_leg, preferred_element_type=f32)
    sketch = jnp.einsum("pyk,pks->pys", far, near, precision=high)
    columns = sketch.shape[0]
    gram_part = jnp.einsum("pys,qys->pq", sketch, sketch, precision=high)
    squeeze_part = jnp.einsum("pys,yjs->pj", sketch, nxt.astype(f32), precision=high)
    both = jnp.concatenate([gram_part, squeeze_part], axis=1)
    total = jnp.sum(gather_all(both.reshape(-1, 128)), axis=0).reshape(both.shape)
    gram = total[:, :columns] / count
    lower = jnp.linalg.cholesky(gram)
    inverse = jax.scipy.linalg.solve_triangular(lower, jnp.eye(columns, dtype=f32), lower=True)
    basis = jnp.einsum("pq,qys->pys", inverse, sketch, precision=high)
    squeezed = jnp.dot(inverse, total[:, columns:], precision=high) / jnp.sqrt(jnp.float32(count))
    return jnp.transpose(basis, (0, 2, 1)), squeezed


def solution(mesh):
    return jax.shard_map(
        per_device,
        mesh=mesh,
        in_specs=(
            P("rows", None, None),
            P("rows", None, None),
            P(BOTH, None, None),
            P(),
            P("rows", "cols"),
        ),
        out_specs=(P(None, BOTH, None), P()),
        check_vma=False,
    )
```

```python
import functools

import jax
import jax.numpy as jnp
from jax import lax
from jax.experimental import pallas as pl
from jax.experimental.pallas import tpu as pltpu
from jax.sharding import PartitionSpec as P

BOTH = ("rows", "cols")
F32, BF16 = jnp.float32, jnp.bfloat16
LANES = 128
VMEM = pl.BlockSpec(memory_space=pltpu.VMEM)
HBM = pl.BlockSpec(memory_space=pltpu.HBM)
NT = (((1,), (1,)), ((), ()))


def iota(shape, axis):
    return lax.broadcasted_iota(jnp.int32, shape, axis)


def halves(value):
    high = value.astype(BF16)
    return high, (value - high.astype(F32)).astype(BF16)


def params(mib):
    return pltpu.CompilerParams(vmem_limit_bytes=mib << 20)


def far_kernel(rows_ref, b_ref, a_ref, out_ref, own_ref, buf, sems, own_sem):
    pairs, used, _ = b_ref.shape
    chunks = sems.shape[0]
    step = pairs // chunks
    quarter = own_ref.shape[2]
    start = pl.multiple_of(lax.axis_index("cols") * quarter, LANES)

    def fetch(c):
        part = pl.ds(c * step, step)
        return pltpu.make_async_copy(b_ref.at[part], buf.at[part], sems.at[c])

    for c in range(chunks):
        fetch(c).start()
    own_copy = pltpu.make_async_copy(a_ref.at[:, :, pl.ds(start, quarter)], own_ref, own_sem)
    own_copy.start()
    own, lanes = out_ref.shape[1:]
    out_ref[:, :, used:] = jnp.zeros((pairs, own, lanes - used), F32)
    for c in range(chunks):
        fetch(c).wait()
        for i in range(step):
            pair = c * step + i
            out_ref[pair, :, :used] = lax.dot_general(rows_ref[...], buf[pair], NT, preferred_element_type=F32)
    own_copy.wait()


def far_sum(rows_t, b_pairs, a_t, quarter):
    pairs, used, depth = b_pairs.shape
    chunks = pairs // 2
    own = rows_t.shape[0]
    return pl.pallas_call(
        far_kernel,
        in_specs=[VMEM, HBM, HBM],
        out_specs=[VMEM, VMEM],
        out_shape=[jax.ShapeDtypeStruct((pairs, own, LANES), F32), jax.ShapeDtypeStruct(a_t.shape[:2] + (quarter,), BF16)],
        scratch_shapes=[pltpu.VMEM((pairs, used, depth), BF16), pltpu.SemaphoreType.DMA((chunks,)), pltpu.SemaphoreType.DMA],
        cost_estimate=pl.CostEstimate(flops=2 * own * pairs * used * depth, bytes_accessed=2 * pairs * used * depth, transcendentals=0),
        compiler_params=params(16),
        name="far_sum",
    )(rows_t, b_pairs, a_t)


def near_kernel(leg_ref, a_ref, high_ref, low_ref):
    columns, width = leg_ref.shape
    _, bond, quarter = a_ref.shape
    deep = 16
    wide = width * deep
    spread = (iota((width, wide), 1) // deep == iota((width, wide), 0)).astype(BF16)
    tiled = jnp.dot(leg_ref[...], spread, preferred_element_type=F32)
    tiled = jnp.broadcast_to(tiled[:, None, :], (columns, deep, wide)).reshape(columns * deep, wide)
    same = iota(tiled.shape, 1) % deep == iota(tiled.shape, 0) % deep
    weights = jnp.where(same, tiled, 0.0).astype(BF16)
    for first in range(0, bond, deep):
        part = a_ref[:, first:first + deep, :].reshape(wide, quarter)
        high, low = halves(jnp.dot(weights, part, preferred_element_type=F32))
        high_ref[:, first:first + deep, :] = high.reshape(columns, deep, quarter)
        low_ref[:, first:first + deep, :] = low.reshape(columns, deep, quarter)


def near_sums(leg_t, a_own):
    width, bond, quarter = a_own.shape
    columns = leg_t.shape[0]
    shape = jax.ShapeDtypeStruct((columns, bond, quarter), BF16)
    return pl.pallas_call(
        near_kernel,
        in_specs=[VMEM, VMEM],
        out_specs=[VMEM, VMEM],
        out_shape=[shape, shape],
        cost_estimate=pl.CostEstimate(flops=32 * columns * bond * width * quarter, bytes_accessed=2 * width * bond * quarter, transcendentals=0),
        compiler_params=params(16),
        name="near_sums",
    )(leg_t, a_own)


def piece_kernel(parts_ref, out_ref):
    piece = jnp.sum(parts_ref[...], axis=0)
    for i in range(out_ref.shape[0]):
        out_ref[i] = piece


def piece_copies(parts, copies):
    return pl.pallas_call(
        piece_kernel,
        in_specs=[VMEM],
        out_specs=VMEM,
        out_shape=jax.ShapeDtypeStruct((copies,) + parts.shape[1:], F32),
        compiler_params=params(8),
        name="piece_copies",
    )(parts)


def sketch_kernel(own_ref, other_ref, near_high_ref, near_low_ref, next_ref, high_ref, low_ref, sums_ref, sketch, high_buf, low_buf, sems):
    groups, own = own_ref.shape[1], own_ref.shape[3]
    columns, bond, quarter = near_high_ref.shape
    pairs = sketch.shape[1]
    width = 2 * pairs
    wide = own * bond
    parity = lax.axis_index("cols") % 2
    lane = iota((LANES, wide), 1) % bond
    keep = [(iota((LANES, wide), 0) == lane + half * bond).astype(BF16) for half in range(2)]
    same = iota((pairs * own, wide), 1) // bond == iota((pairs * own, wide), 0) % own

    def group(far_ref, odd, g, carry):
        far = far_ref[:, g].reshape(-1, LANES)[:pairs * own]
        parts = []
        for piece in halves(far):
            spread = [jnp.dot(piece, keep[half], preferred_element_type=F32) for half in range(2)]
            parts.append(jnp.concatenate([jnp.where(same, s, 0.0).astype(BF16) for s in spread], axis=0))
        first = pl.multiple_of((2 * g + odd) * own, own)
        near_high = near_high_ref[pl.ds(first, own)].reshape(wide, quarter)
        near_low = near_low_ref[pl.ds(first, own)].reshape(wide, quarter)
        left = jnp.concatenate([parts[0], parts[1], parts[0]], axis=1)
        right = jnp.concatenate([near_high, near_high, near_low], axis=0)
        result = jnp.dot(left, right, preferred_element_type=F32)
        sketch[:, :, pl.ds(first, own), :] = result.reshape(2, pairs, own, quarter)
        return carry

    lax.fori_loop(0, groups, functools.partial(group, own_ref, parity), 0)
    lax.fori_loop(0, groups, functools.partial(group, other_ref, 1 - parity), 0)

    def store(i, which):
        source, target = ((high_buf, high_ref), (low_buf, low_ref))[which]
        part = pl.ds(pl.multiple_of(8 * i, 8), 8)
        return pltpu.make_async_copy(source.at[part], target.at[part], sems.at[which, i])

    def products(i, total):
        for step in range(4):
            for half in range(2):
                y = 8 * i + 2 * step + half
                high, low = halves(sketch[half, 4 * i + step])
                high_buf[y] = high
                low_buf[y] = low
                both = jnp.concatenate([high, low], axis=0)
                left = jnp.concatenate([both, next_ref[y]], axis=0)
                total = total + lax.dot_general(left, both, NT, preferred_element_type=F32)
        store(i, 0).start()
        store(i, 1).start()
        return total

    rows = 2 * columns + bond
    total = lax.fori_loop(0, width // 8, products, jnp.zeros((rows, 2 * columns), F32))
    square = jnp.zeros((LANES, LANES), F32)
    padded = jnp.concatenate([jnp.concatenate([total, jnp.zeros((rows, LANES - 2 * columns), F32)], axis=1), square[rows:]], axis=0)
    turned = padded.T
    summed = turned[:columns] + turned[columns:2 * columns]
    gram = summed[:, :columns] + summed[:, columns:2 * columns]
    squeeze = summed[:, 2 * columns:rows]
    flat = jnp.concatenate([v[8 * i:8 * i + 8] for v in (gram, squeeze) for i in range(columns // 8)], axis=1)
    blocks = fold(flat)
    for copy in range(sums_ref.shape[0]):
        for i, block in enumerate(blocks):
            sums_ref[copy, i] = block
    for i in range(width // 8):
        store(i, 0).wait()
        store(i, 1).wait()


def fold(flat):
    blocks = []
    whole = flat.shape[1] // LANES * LANES
    for i in range(0, whole, LANES):
        blocks += [flat[:4, i:i + LANES], flat[4:, i:i + LANES]]
    if whole < flat.shape[1]:
        blocks.append(jnp.concatenate([flat[:4, whole:], flat[4:, whole:]], axis=1))
    return blocks


def unfold(blocks):
    flat = [jnp.concatenate(blocks[i:i + 2], axis=0) for i in range(0, len(blocks) - 1, 2)]
    if len(blocks) % 2:
        last = blocks[-1]
        flat.append(jnp.concatenate([last[:, :LANES // 2], last[:, LANES // 2:]], axis=0))
    return jnp.concatenate(flat, axis=1)


def sketch_products(far_own, far_other, near_high, near_low, nxt, copies):
    columns, bond, quarter = near_high.shape
    width = nxt.shape[0]
    shape = jax.ShapeDtypeStruct((width, columns, quarter), BF16)
    blocks = columns * (columns + bond) // 512
    held = pltpu.VMEM((width, columns, quarter), BF16)
    return pl.pallas_call(
        sketch_kernel,
        in_specs=[VMEM] * 5,
        out_specs=[HBM, HBM, VMEM],
        out_shape=[shape, shape, jax.ShapeDtypeStruct((copies, blocks, 4, LANES), F32)],
        scratch_shapes=[pltpu.VMEM((2, width // 2, columns, quarter), F32), held, held, pltpu.SemaphoreType.DMA((2, width // 8))],
        cost_estimate=pl.CostEstimate(flops=2 * columns * bond * width * quarter * 24, bytes_accessed=8 * columns * width * quarter, transcendentals=0),
        compiler_params=params(16),
        name="sketch_products",
    )(far_own, far_other, near_high, near_low, nxt)


def basis_kernel(count, sums_ref, high_ref, low_ref, basis_ref, squeezed_ref, square, high_buf, low_buf, out, in_sems, out_sems):
    width, columns, quarter = high_ref.shape
    bond = squeezed_ref.shape[1]

    def fetch(g, which):
        source, target = ((high_ref, high_buf), (low_ref, low_buf))[which]
        part = pl.ds(pl.multiple_of(8 * g, 8), 8)
        return pltpu.make_async_copy(source.at[part], target.at[part], in_sems.at[which, g])

    def store(g):
        return pltpu.make_async_copy(out.at[g], basis_ref.at[:, pl.ds(pl.multiple_of(8 * g, 8), 8), :], out_sems.at[g])

    for g in range(width // 8):
        fetch(g, 0).start()
        fetch(g, 1).start()
    summed = jnp.sum(sums_ref[...], axis=0)
    flat = unfold([summed[i] for i in range(summed.shape[0])])
    square[...] = jnp.zeros_like(square)
    for i in range(columns // 8):
        square[8 * i:8 * i + 8, :columns] = flat[:, i * columns:(i + 1) * columns] / count
        first = columns * (columns // 8) + i * bond
        square[8 * i:8 * i + 8, columns:columns + bond] = flat[:, first:first + bond]
    matrix = square[...]
    wide = 8 * columns
    unit = (iota((columns, wide), 1) % columns == iota((columns, wide), 0)).astype(F32)
    row = iota((columns, LANES), 0)
    roots = jnp.zeros((columns, LANES), F32)
    block = 4
    for first in range(0, columns, block):
        cols = [jnp.broadcast_to(matrix[:, first + j:first + j + 1], (columns, LANES)) for j in range(block)]
        for j in range(block):
            k = first + j
            pivot = cols[j][k:k + 1]
            factor = jnp.where(row > k, cols[j] * (1.0 / pivot), 0.0)
            for i in range(j + 1, block):
                cols[i] = cols[i] - factor * cols[i][k:k + 1]
            matrix = matrix - factor * matrix[k:k + 1]
            unit = unit - jnp.concatenate([factor] * (wide // LANES), axis=1) * unit[k:k + 1]
            roots = jnp.where(row == k, 1.0 / jnp.sqrt(pivot), roots)
    squeezed_ref[...] = (matrix * roots)[:, columns:columns + bond] / count ** 0.5
    inverse = unit * jnp.concatenate([roots] * (wide // LANES), axis=1)
    spread = jnp.broadcast_to(inverse[:, None, :], (columns, 8, wide)).reshape(wide, wide)
    same = iota((wide, wide), 1) // columns == iota((wide, wide), 0) % 8
    left_high, left_low = halves(jnp.where(same, spread, 0.0))

    def group(g, carry):
        fetch(g, 0).wait()
        fetch(g, 1).wait()
        first = pl.multiple_of(8 * g, 8)
        high = high_buf[pl.ds(first, 8)].reshape(wide, quarter)
        low = low_buf[pl.ds(first, 8)].reshape(wide, quarter)
        result = jnp.dot(left_high, high, preferred_element_type=F32)
        result += jnp.dot(left_low, high, preferred_element_type=F32)
        result += jnp.dot(left_high, low, preferred_element_type=F32)
        out[g] = result.reshape(columns, 8, quarter)
        store(g).start()
        return carry

    lax.fori_loop(0, width // 8, group, 0)
    lax.fori_loop(0, width // 8, lambda g, carry: (store(g).wait(), carry)[1], 0)


def basis_of(sums, high, low, bond, count):
    width, columns, quarter = high.shape
    held = pltpu.VMEM((width, columns, quarter), BF16)
    return pl.pallas_call(
        functools.partial(basis_kernel, float(count)),
        in_specs=[VMEM, HBM, HBM],
        out_specs=[HBM, VMEM],
        out_shape=[jax.ShapeDtypeStruct((columns, width, quarter), F32), jax.ShapeDtypeStruct((columns, bond), F32)],
        scratch_shapes=[
            pltpu.VMEM((columns, LANES), F32),
            held,
            held,
            pltpu.VMEM((width // 8, columns, 8, quarter), F32),
            pltpu.SemaphoreType.DMA((2, width // 8)),
            pltpu.SemaphoreType.DMA((width // 8,)),
        ],
        cost_estimate=pl.CostEstimate(flops=2 * columns * columns * width * quarter * 24, bytes_accessed=4 * columns * width * quarter, transcendentals=0),
        compiler_params=params(16),
        name="basis_of",
    )(sums, high, low)


def per_device(factor_a, factor_b, next_factor, sketch_leg, sketch_rows):
    rows, cols = lax.axis_size("rows"), lax.axis_size("cols")
    devices = rows * cols
    local_rows, width, bond = factor_a.shape
    quarter = local_rows // cols
    count = local_rows * rows * width
    a = jnp.transpose(factor_a, (1, 2, 0))
    b = jnp.transpose(factor_b, (1, 2, 0)).reshape(width // 2, 2 * bond, local_rows)
    nxt = jnp.transpose(next_factor, (1, 2, 0))
    own = sketch_rows.shape[1]
    b, a = (pltpu.with_memory_space_constraint(v, pltpu.HBM) for v in (b, a))
    partial, a_own = far_sum(sketch_rows.T, b, a, quarter)
    each = -(-(width // 2) // rows)
    partial = jnp.pad(partial, ((0, each * rows - width // 2), (0, 0), (0, 0))).reshape(rows, each, own, LANES)
    parts = lax.all_to_all(partial, "rows", 0, 0)
    parities = [[i for i in range(devices) if i % 2 == parity] for parity in range(2)]
    pieces = lax.all_to_all(piece_copies(parts, devices // 2), BOTH, 0, 0, axis_index_groups=parities)
    far_own = pieces.reshape(rows, cols // 2, each, own, LANES)
    far_other = lax.ppermute(far_own, "cols", [(i, i ^ 1) for i in range(cols)])
    near_high, near_low = near_sums(sketch_leg.T, a_own)
    high, low, sums = sketch_products(far_own, far_other, near_high, near_low, nxt, devices)
    basis, squeezed = basis_of(lax.all_to_all(sums, BOTH, 0, 0), high, low, bond, count)
    return jnp.transpose(basis, (0, 2, 1)), squeezed


def solution(mesh):
    return jax.shard_map(
        per_device,
        mesh=mesh,
        in_specs=(
            P("rows", None, None),
            P("rows", None, None),
            P(BOTH, None, None),
            P(),
            P("rows", "cols"),
        ),
        out_specs=(P(None, BOTH, None), P()),
        check_vma=False,
    )
```

```python
import functools

import jax
import jax.numpy as jnp
from jax import lax
from jax.experimental import pallas as pl
from jax.experimental.pallas import tpu as pltpu
from jax.sharding import PartitionSpec as P

BOTH = ("rows", "cols")
F32, BF16 = jnp.float32, jnp.bfloat16
LANES = 128
VMEM = pl.BlockSpec(memory_space=pltpu.VMEM)
HBM = pl.BlockSpec(memory_space=pltpu.HBM)
NT = (((1,), (1,)), ((), ()))


def iota(shape, axis):
    return lax.broadcasted_iota(jnp.int32, shape, axis)


def halves(value):
    high = value.astype(BF16)
    return high, (value - high.astype(F32)).astype(BF16)


def params(mib):
    return pltpu.CompilerParams(vmem_limit_bytes=mib << 20)


def far_kernel(rows_ref, b_ref, a_ref, out_ref, own_ref, rows_buf, buf, rows_sem, own_sem, sems):
    pairs, used, _ = b_ref.shape
    chunks = sems.shape[0]
    step = pairs // chunks
    quarter = own_ref.shape[2]
    start = pl.multiple_of(lax.axis_index("cols") * quarter, LANES)

    def fetch(c):
        part = pl.ds(c * step, step)
        return pltpu.make_async_copy(b_ref.at[part], buf.at[part], sems.at[c])

    rows_copy = pltpu.make_async_copy(rows_ref, rows_buf, rows_sem)
    rows_copy.start()
    ahead = 2
    for c in range(ahead):
        fetch(c).start()
    own_copy = pltpu.make_async_copy(a_ref.at[:, :, pl.ds(start, quarter)], own_ref, own_sem)
    own, lanes = out_ref.shape[1:]
    out_ref[:, :, used:] = jnp.zeros((pairs, own, lanes - used), F32)
    rows_copy.wait()
    for c in range(ahead, chunks):
        fetch(c).start()
    own_copy.start()
    for c in range(chunks):
        fetch(c).wait()
        for i in range(step):
            pair = c * step + i
            out_ref[pair, :, :used] = lax.dot_general(rows_buf[...], buf[pair], NT, preferred_element_type=F32)
    own_copy.wait()


def far_sum(rows_t, b_pairs, a_t, quarter):
    pairs, used, depth = b_pairs.shape
    chunks = pairs // 6
    own = rows_t.shape[0]
    return pl.pallas_call(
        far_kernel,
        in_specs=[HBM] * 3,
        out_specs=[VMEM] * 2,
        out_shape=[jax.ShapeDtypeStruct((pairs, own, LANES), F32), jax.ShapeDtypeStruct(a_t.shape[:2] + (quarter,), BF16)],
        scratch_shapes=[
            pltpu.VMEM(rows_t.shape, BF16),
            pltpu.VMEM((pairs, used, depth), BF16),
            pltpu.SemaphoreType.DMA,
            pltpu.SemaphoreType.DMA,
            pltpu.SemaphoreType.DMA((chunks,)),
        ],
        cost_estimate=pl.CostEstimate(flops=2 * own * pairs * used * depth, bytes_accessed=2 * pairs * used * depth, transcendentals=0),
        compiler_params=params(16),
        name="far_sum",
    )(rows_t, b_pairs, a_t)


def near_kernel(leg_ref, a_ref, high_ref, low_ref):
    columns, width = leg_ref.shape
    _, bond, quarter = high_ref.shape
    deep = 16
    wide = width * deep
    spread = (iota((width, wide), 1) // deep == iota((width, wide), 0)).astype(BF16)
    tiled = jnp.dot(leg_ref[...], spread, preferred_element_type=F32)
    tiled = jnp.broadcast_to(tiled[:, None, :], (columns, deep, wide)).reshape(columns * deep, wide)
    same = iota(tiled.shape, 1) % deep == iota(tiled.shape, 0) % deep
    weights = jnp.where(same, tiled, 0.0).astype(BF16)
    for first in range(0, bond, deep):
        part = a_ref[:, first:first + deep, :].reshape(wide, quarter)
        high, low = halves(jnp.dot(weights, part, preferred_element_type=F32))
        high_ref[:, first:first + deep, :] = high.reshape(columns, deep, quarter)
        low_ref[:, first:first + deep, :] = low.reshape(columns, deep, quarter)


def near_sums(leg_t, a_own):
    width, bond, quarter = a_own.shape
    columns = leg_t.shape[0]
    shape = jax.ShapeDtypeStruct((columns, bond, quarter), BF16)
    return pl.pallas_call(
        near_kernel,
        in_specs=[VMEM, VMEM],
        out_specs=[VMEM, VMEM],
        out_shape=[shape, shape],
        cost_estimate=pl.CostEstimate(flops=32 * columns * bond * width * quarter, bytes_accessed=2 * width * bond * quarter, transcendentals=0),
        compiler_params=params(16),
        name="near_sums",
    )(leg_t, a_own)


def piece_kernel(parts_ref, out_ref):
    piece = jnp.sum(parts_ref[...], axis=0)
    for i in range(out_ref.shape[0]):
        out_ref[i] = piece


def piece_copies(parts, copies):
    return pl.pallas_call(
        piece_kernel,
        in_specs=[VMEM],
        out_specs=VMEM,
        out_shape=jax.ShapeDtypeStruct((copies,) + parts.shape[1:], F32),
        compiler_params=params(8),
        name="piece_copies",
    )(parts)


def sketch_kernel(own_ref, other_ref, near_high_ref, near_low_ref, next_ref, high_ref, low_ref, sums_ref, sketch):
    groups, own = own_ref.shape[1], own_ref.shape[3]
    columns, bond, quarter = near_high_ref.shape
    pairs = sketch.shape[1]
    width = 2 * pairs
    wide = own * bond
    parity = lax.axis_index("cols") % 2
    lane = iota((LANES, wide), 1) % bond
    keep = [(iota((LANES, wide), 0) == lane + half * bond).astype(BF16) for half in range(2)]
    same = iota((pairs * own, wide), 1) // bond == iota((pairs * own, wide), 0) % own

    def group(far_ref, odd, g, carry):
        far = far_ref[:, g].reshape(-1, LANES)[:pairs * own]
        parts = []
        for piece in halves(far):
            spread = [jnp.dot(piece, keep[half], preferred_element_type=F32) for half in range(2)]
            parts.append(jnp.concatenate([jnp.where(same, s, 0.0).astype(BF16) for s in spread], axis=0))
        first = pl.multiple_of((2 * g + odd) * own, own)
        near_high = near_high_ref[pl.ds(first, own)].reshape(wide, quarter)
        near_low = near_low_ref[pl.ds(first, own)].reshape(wide, quarter)
        left = jnp.concatenate([parts[0], parts[1], parts[0]], axis=1)
        right = jnp.concatenate([near_high, near_high, near_low], axis=0)
        result = jnp.dot(left, right, preferred_element_type=F32)
        sketch[:, :, pl.ds(first, own), :] = result.reshape(2, pairs, own, quarter)
        return carry

    lax.fori_loop(0, groups, functools.partial(group, own_ref, parity), 0)
    lax.fori_loop(0, groups, functools.partial(group, other_ref, 1 - parity), 0)

    def products(i, total):
        for step in range(4):
            for half in range(2):
                y = 8 * i + 2 * step + half
                high, low = halves(sketch[half, 4 * i + step])
                high_ref[y] = high
                low_ref[y] = low
                both = jnp.concatenate([high, low], axis=0)
                left = jnp.concatenate([both, next_ref[y]], axis=0)
                total = total + lax.dot_general(left, both, NT, preferred_element_type=F32)
        return total

    rows = 2 * columns + bond
    total = lax.fori_loop(0, width // 8, products, jnp.zeros((rows, 2 * columns), F32))
    square = jnp.zeros((LANES, LANES), F32)
    padded = jnp.concatenate([jnp.concatenate([total, jnp.zeros((rows, LANES - 2 * columns), F32)], axis=1), square[rows:]], axis=0)
    turned = padded.T
    summed = turned[:columns] + turned[columns:2 * columns]
    gram = summed[:, :columns] + summed[:, columns:2 * columns]
    squeeze = summed[:, 2 * columns:rows]
    flat = jnp.concatenate([v[8 * i:8 * i + 8] for v in (gram, squeeze) for i in range(columns // 8)], axis=1)
    blocks = fold(flat)
    for copy in range(sums_ref.shape[0]):
        for i, block in enumerate(blocks):
            sums_ref[copy, i] = block


def fold(flat):
    blocks = []
    whole = flat.shape[1] // LANES * LANES
    for i in range(0, whole, LANES):
        blocks += [flat[:4, i:i + LANES], flat[4:, i:i + LANES]]
    if whole < flat.shape[1]:
        blocks.append(jnp.concatenate([flat[:4, whole:], flat[4:, whole:]], axis=1))
    return blocks


def unfold(blocks):
    flat = [jnp.concatenate(blocks[i:i + 2], axis=0) for i in range(0, len(blocks) - 1, 2)]
    if len(blocks) % 2:
        last = blocks[-1]
        flat.append(jnp.concatenate([last[:, :LANES // 2], last[:, LANES // 2:]], axis=0))
    return jnp.concatenate(flat, axis=1)


def sketch_products(far_own, far_other, near_high, near_low, nxt, copies):
    columns, bond, quarter = near_high.shape
    width = nxt.shape[0]
    shape = jax.ShapeDtypeStruct((width, columns, quarter), BF16)
    blocks = columns * (columns + bond) // 512
    return pl.pallas_call(
        sketch_kernel,
        in_specs=[VMEM] * 5,
        out_specs=[VMEM] * 3,
        out_shape=[shape, shape, jax.ShapeDtypeStruct((copies, blocks, 4, LANES), F32)],
        scratch_shapes=[pltpu.VMEM((2, width // 2, columns, quarter), F32)],
        cost_estimate=pl.CostEstimate(flops=2 * columns * bond * width * quarter * 24, bytes_accessed=8 * columns * width * quarter, transcendentals=0),
        compiler_params=params(16),
        name="sketch_products",
    )(far_own, far_other, near_high, near_low, nxt)


def basis_kernel(count, sums_ref, high_ref, low_ref, basis_ref, squeezed_ref, square, out, out_sems):
    width, columns, quarter = high_ref.shape
    bond = squeezed_ref.shape[1]

    def store(g):
        return pltpu.make_async_copy(out.at[g], basis_ref.at[:, pl.ds(pl.multiple_of(8 * g, 8), 8), :], out_sems.at[g])

    summed = jnp.sum(sums_ref[...], axis=0)
    flat = unfold([summed[i] for i in range(summed.shape[0])])
    square[...] = jnp.zeros_like(square)
    for i in range(columns // 8):
        square[8 * i:8 * i + 8, :columns] = flat[:, i * columns:(i + 1) * columns] / count
        first = columns * (columns // 8) + i * bond
        square[8 * i:8 * i + 8, columns:columns + bond] = flat[:, first:first + bond]
    matrix = square[...]
    wide = 8 * columns
    unit = (iota((columns, wide), 1) % columns == iota((columns, wide), 0)).astype(F32)
    row = iota((columns, LANES), 0)
    roots = jnp.zeros((columns, LANES), F32)
    block = 4
    for first in range(0, columns, block):
        cols = [jnp.broadcast_to(matrix[:, first + j:first + j + 1], (columns, LANES)) for j in range(block)]
        for j in range(block):
            k = first + j
            pivot = cols[j][k:k + 1]
            factor = jnp.where(row > k, cols[j] * (1.0 / pivot), 0.0)
            for i in range(j + 1, block):
                cols[i] = cols[i] - factor * cols[i][k:k + 1]
            matrix = matrix - factor * matrix[k:k + 1]
            unit = unit - jnp.concatenate([factor] * (wide // LANES), axis=1) * unit[k:k + 1]
            roots = jnp.where(row == k, 1.0 / jnp.sqrt(pivot), roots)
    squeezed_ref[...] = (matrix * roots)[:, columns:columns + bond] / count ** 0.5
    inverse = unit * jnp.concatenate([roots] * (wide // LANES), axis=1)
    spread = jnp.broadcast_to(inverse[:, None, :], (columns, 8, wide)).reshape(wide, wide)
    same = iota((wide, wide), 1) // columns == iota((wide, wide), 0) % 8
    left_high, left_low = halves(jnp.where(same, spread, 0.0))

    def group(g, carry):
        first = pl.multiple_of(8 * g, 8)
        high = high_ref[pl.ds(first, 8)].reshape(wide, quarter)
        low = low_ref[pl.ds(first, 8)].reshape(wide, quarter)
        result = jnp.dot(left_high, high, preferred_element_type=F32)
        result += jnp.dot(left_low, high, preferred_element_type=F32)
        result += jnp.dot(left_high, low, preferred_element_type=F32)
        out[g] = result.reshape(columns, 8, quarter)
        store(g).start()
        return carry

    lax.fori_loop(0, width // 8, group, 0)
    lax.fori_loop(0, width // 8, lambda g, carry: (store(g).wait(), carry)[1], 0)


def basis_of(sums, high, low, bond, count):
    width, columns, quarter = high.shape
    return pl.pallas_call(
        functools.partial(basis_kernel, float(count)),
        in_specs=[VMEM] * 3,
        out_specs=[HBM, VMEM],
        out_shape=[jax.ShapeDtypeStruct((columns, width, quarter), F32), jax.ShapeDtypeStruct((columns, bond), F32)],
        scratch_shapes=[
            pltpu.VMEM((columns, LANES), F32),
            pltpu.VMEM((width // 8, columns, 8, quarter), F32),
            pltpu.SemaphoreType.DMA((width // 8,)),
        ],
        cost_estimate=pl.CostEstimate(flops=2 * columns * columns * width * quarter * 24, bytes_accessed=4 * columns * width * quarter, transcendentals=0),
        compiler_params=params(16),
        name="basis_of",
    )(sums, high, low)


def per_device(factor_a, factor_b, next_factor, sketch_leg, sketch_rows):
    rows, cols = lax.axis_size("rows"), lax.axis_size("cols")
    devices = rows * cols
    local_rows, width, bond = factor_a.shape
    quarter = local_rows // cols
    count = local_rows * rows * width
    a = jnp.transpose(factor_a, (1, 2, 0))
    b = jnp.transpose(factor_b, (1, 2, 0)).reshape(width // 2, 2 * bond, local_rows)
    nxt = jnp.transpose(next_factor, (1, 2, 0))
    own = sketch_rows.shape[1]
    operands = [pltpu.with_memory_space_constraint(v, pltpu.HBM) for v in (sketch_rows.T, b, a)]
    partial, a_own = far_sum(*operands, quarter)
    each = -(-(width // 2) // rows)
    partial = jnp.pad(partial, ((0, each * rows - width // 2), (0, 0), (0, 0))).reshape(rows, each, own, LANES)
    parts = lax.all_to_all(partial, "rows", 0, 0)
    parities = [[i for i in range(devices) if i % 2 == parity] for parity in range(2)]
    pieces = lax.all_to_all(piece_copies(parts, devices // 2), BOTH, 0, 0, axis_index_groups=parities)
    far_own = pieces.reshape(rows, cols // 2, each, own, LANES)
    far_other = lax.ppermute(far_own, "cols", [(i, i ^ 1) for i in range(cols)])
    near_high, near_low = near_sums(sketch_leg.T, a_own)
    high, low, sums = sketch_products(far_own, far_other, near_high, near_low, nxt, devices)
    basis, squeezed = basis_of(lax.all_to_all(sums, BOTH, 0, 0), high, low, bond, count)
    return jnp.transpose(basis, (0, 2, 1)), squeezed


def solution(mesh):
    return jax.shard_map(
        per_device,
        mesh=mesh,
        in_specs=(
            P("rows", None, None),
            P("rows", None, None),
            P(BOTH, None, None),
            P(),
            P("rows", "cols"),
        ),
        out_specs=(P(None, BOTH, None), P()),
        check_vma=False,
    )
```

```python
import functools

import jax
import jax.numpy as jnp
from jax import lax
from jax.experimental import pallas as pl
from jax.experimental.pallas import tpu as pltpu
from jax.sharding import PartitionSpec as P

BOTH = ("rows", "cols")
F32, BF16 = jnp.float32, jnp.bfloat16
LANES = 128
VMEM = pl.BlockSpec(memory_space=pltpu.VMEM)
HBM = pl.BlockSpec(memory_space=pltpu.HBM)
NT = (((1,), (1,)), ((), ()))


def iota(shape, axis):
    return lax.broadcasted_iota(jnp.int32, shape, axis)


def halves(value):
    high = value.astype(BF16)
    return high, (value - high.astype(F32)).astype(BF16)


def params(mib):
    return pltpu.CompilerParams(vmem_limit_bytes=mib << 20)


def far_kernel(rows_ref, b_ref, a_ref, out_ref, own_ref, rows_buf, buf, rows_sem, own_sem, sems):
    pairs, used, _ = b_ref.shape
    chunks = sems.shape[0]
    step = pairs // chunks
    quarter = own_ref.shape[2]
    start = pl.multiple_of(lax.axis_index("cols") * quarter, LANES)

    def fetch(c):
        part = pl.ds(c * step, step)
        return pltpu.make_async_copy(b_ref.at[part], buf.at[part], sems.at[c])

    rows_copy = pltpu.make_async_copy(rows_ref, rows_buf, rows_sem)
    rows_copy.start()
    ahead = 2
    for c in range(ahead):
        fetch(c).start()
    own_copy = pltpu.make_async_copy(a_ref.at[:, :, pl.ds(start, quarter)], own_ref, own_sem)
    own, lanes = out_ref.shape[1:]
    out_ref[:, :, used:] = jnp.zeros((pairs, own, lanes - used), F32)
    rows_copy.wait()
    for c in range(ahead, chunks):
        fetch(c).start()
    own_copy.start()
    for c in range(chunks):
        fetch(c).wait()
        for i in range(step):
            pair = c * step + i
            out_ref[pair, :, :used] = lax.dot_general(rows_buf[...], buf[pair], NT, preferred_element_type=F32)
    own_copy.wait()


def far_sum(rows_t, b_pairs, a_t, quarter):
    pairs, used, depth = b_pairs.shape
    chunks = pairs // 6
    own = rows_t.shape[0]
    return pl.pallas_call(
        far_kernel,
        in_specs=[HBM] * 3,
        out_specs=[VMEM] * 2,
        out_shape=[jax.ShapeDtypeStruct((pairs, own, LANES), F32), jax.ShapeDtypeStruct(a_t.shape[:2] + (quarter,), BF16)],
        scratch_shapes=[
            pltpu.VMEM(rows_t.shape, BF16),
            pltpu.VMEM((pairs, used, depth), BF16),
            pltpu.SemaphoreType.DMA,
            pltpu.SemaphoreType.DMA,
            pltpu.SemaphoreType.DMA((chunks,)),
        ],
        cost_estimate=pl.CostEstimate(flops=2 * own * pairs * used * depth, bytes_accessed=2 * pairs * used * depth, transcendentals=0),
        compiler_params=params(16),
        name="far_sum",
    )(rows_t, b_pairs, a_t)


def near_kernel(leg_ref, a_ref, high_ref, low_ref):
    columns, width = leg_ref.shape
    _, bond, quarter = high_ref.shape
    deep = 16
    wide = width * deep
    spread = (iota((width, wide), 1) // deep == iota((width, wide), 0)).astype(BF16)
    tiled = jnp.dot(leg_ref[...], spread, preferred_element_type=F32)
    tiled = jnp.broadcast_to(tiled[:, None, :], (columns, deep, wide)).reshape(columns * deep, wide)
    same = iota(tiled.shape, 1) % deep == iota(tiled.shape, 0) % deep
    weights = jnp.where(same, tiled, 0.0).astype(BF16)
    for first in range(0, bond, deep):
        part = a_ref[:, first:first + deep, :].reshape(wide, quarter)
        high, low = halves(jnp.dot(weights, part, preferred_element_type=F32))
        high_ref[:, first:first + deep, :] = high.reshape(columns, deep, quarter)
        low_ref[:, first:first + deep, :] = low.reshape(columns, deep, quarter)


def near_sums(leg_t, a_own):
    width, bond, quarter = a_own.shape
    columns = leg_t.shape[0]
    shape = jax.ShapeDtypeStruct((columns, bond, quarter), BF16)
    return pl.pallas_call(
        near_kernel,
        in_specs=[VMEM, VMEM],
        out_specs=[VMEM, VMEM],
        out_shape=[shape, shape],
        cost_estimate=pl.CostEstimate(flops=32 * columns * bond * width * quarter, bytes_accessed=2 * width * bond * quarter, transcendentals=0),
        compiler_params=params(16),
        name="near_sums",
    )(leg_t, a_own)


def piece_kernel(bond, parts_ref, out_ref):
    piece = jnp.sum(parts_ref[...], axis=0)
    half = piece.shape[1] // 2
    crossed = pltpu.roll(piece, half, 1)
    upper = iota(piece.shape, 1) < half
    left = iota(piece.shape, 2) < bond
    crossed = jnp.where(upper, pltpu.roll(crossed, bond, 2), pltpu.roll(crossed, LANES - bond, 2))
    piece = jnp.where(upper == left, piece, crossed)
    for i in range(out_ref.shape[0]):
        out_ref[i] = piece


def piece_copies(parts, copies, bond):
    return pl.pallas_call(
        functools.partial(piece_kernel, bond),
        in_specs=[VMEM],
        out_specs=VMEM,
        out_shape=jax.ShapeDtypeStruct((copies,) + parts.shape[1:], F32),
        compiler_params=params(8),
        name="piece_copies",
    )(parts)


def sketch_kernel(own_ref, other_ref, near_high_ref, near_low_ref, next_ref, high_ref, low_ref, sums_ref, sketch):
    groups, own = own_ref.shape[1], own_ref.shape[3]
    columns, bond, quarter = near_high_ref.shape
    pairs = sketch.shape[0]
    part = own // 2
    wide = part * bond
    parity = lax.axis_index("cols") % 2
    lane = iota((LANES, wide), 1) % bond
    keep = [(iota((LANES, wide), 0) == lane + half * bond).astype(BF16) for half in range(2)]
    same = iota((pairs * own, wide), 1) // bond == iota((pairs * own, wide), 0) % part

    def group(far_ref, odd, g, carry):
        far = halves(far_ref[:, g].reshape(-1, LANES)[:pairs * own])
        for half in range(2):
            spread = [jnp.dot(piece, keep[half], preferred_element_type=F32) for piece in far]
            high, low = (jnp.where(same, value, 0.0).astype(BF16) for value in spread)
            block = 2 * (2 * g + odd) + half
            near_high = near_high_ref[pl.ds(block * part, part)].reshape(wide, quarter)
            near_low = near_low_ref[pl.ds(block * part, part)].reshape(wide, quarter)
            both = jnp.dot(jnp.concatenate([high, low], axis=0), near_high, preferred_element_type=F32)
            result = both[:pairs * own] + both[pairs * own:] + jnp.dot(high, near_low, preferred_element_type=F32)
            sketch[:, pl.ds(pl.multiple_of(block * own, own), own), :] = result.reshape(pairs, own, quarter)
        return carry

    lax.fori_loop(0, groups, functools.partial(group, own_ref, parity), 0)
    lax.fori_loop(0, groups, functools.partial(group, other_ref, 1 - parity), 0)

    def products(i, total):
        for step in range(4):
            pair = 4 * i + step
            high, low = halves(sketch[pair])
            high_ref[pair] = high
            low_ref[pair] = low
            left = jnp.concatenate([high, next_ref[2 * pair], next_ref[2 * pair + 1]], axis=0)
            total = total + lax.dot_general(left, jnp.concatenate([high, low], axis=0), NT, preferred_element_type=F32)
        return total

    doubled = 2 * columns
    rows = doubled + 2 * bond
    total = lax.fori_loop(0, pairs // 4, products, jnp.zeros((rows, LANES), F32))
    row, lane = iota((rows, LANES), 0), iota((rows, LANES), 1)
    row_y = jnp.where(row < doubled, row // part % 2, (row >= doubled + bond).astype(jnp.int32))
    total = jnp.where(row_y == lane // part % 2, total, 0.0)
    lane, target = iota((LANES, doubled), 0), iota((LANES, doubled), 1)
    column = lane % doubled // own * part + lane % part
    pick = (column == target % columns) & ((target < columns) | (lane >= doubled))
    packed = jnp.dot(total, pick.astype(F32), preferred_element_type=F32, precision=lax.Precision.HIGHEST)
    squares = packed[:doubled].reshape(doubled // own, own, doubled)
    squares = squares + pltpu.roll(squares, part, 1)
    upper = iota((own, doubled), 0) < part
    squares = jnp.concatenate([jnp.where(upper, squares[2 * i], squares[2 * i + 1]) for i in range(columns // own)], axis=0)
    squeezes = packed[doubled:doubled + bond] + packed[doubled + bond:]
    padded = jnp.concatenate([squares, squeezes, jnp.zeros((LANES - columns - bond, doubled), F32)], axis=0)
    padded = jnp.concatenate([padded, jnp.zeros((LANES, LANES - doubled), F32)], axis=1)
    turned = padded.T
    gram = squares[:, :columns] + turned[columns:doubled, :columns]
    squeeze = turned[:columns, columns:columns + bond]
    flat = jnp.concatenate([v[8 * i:8 * i + 8] for v in (gram, squeeze) for i in range(columns // 8)], axis=1)
    blocks = fold(flat)
    for i, block in enumerate(blocks):
        sums_ref[i] = block


def fold(flat):
    blocks = []
    whole = flat.shape[1] // LANES * LANES
    for i in range(0, whole, LANES):
        blocks += [flat[:4, i:i + LANES], flat[4:, i:i + LANES]]
    if whole < flat.shape[1]:
        blocks.append(jnp.concatenate([flat[:4, whole:], flat[4:, whole:]], axis=1))
    return blocks


def unfold(blocks):
    flat = [jnp.concatenate(blocks[i:i + 2], axis=0) for i in range(0, len(blocks) - 1, 2)]
    if len(blocks) % 2:
        last = blocks[-1]
        flat.append(jnp.concatenate([last[:, :LANES // 2], last[:, LANES // 2:]], axis=0))
    return jnp.concatenate(flat, axis=1)


def sketch_products(far_own, far_other, near_high, near_low, nxt):
    columns, bond, quarter = near_high.shape
    width = nxt.shape[0]
    shape = jax.ShapeDtypeStruct((width // 2, 2 * columns, quarter), BF16)
    blocks = columns * (columns + bond) // 512
    return pl.pallas_call(
        sketch_kernel,
        in_specs=[VMEM] * 5,
        out_specs=[VMEM] * 3,
        out_shape=[shape, shape, jax.ShapeDtypeStruct((blocks, 4, LANES), F32)],
        scratch_shapes=[pltpu.VMEM((width // 2, 2 * columns, quarter), F32)],
        cost_estimate=pl.CostEstimate(flops=2 * columns * bond * width * quarter * 24, bytes_accessed=8 * columns * width * quarter, transcendentals=0),
        compiler_params=params(16),
        name="sketch_products",
    )(far_own, far_other, near_high, near_low, nxt)


def pair_kernel(mine_ref, other_ref, out_ref):
    both = mine_ref[...] + other_ref[...]
    for i in range(out_ref.shape[0]):
        out_ref[i] = both


def pair_copies(mine, other, copies):
    return pl.pallas_call(
        pair_kernel,
        in_specs=[VMEM] * 2,
        out_specs=VMEM,
        out_shape=jax.ShapeDtypeStruct((copies,) + mine.shape, F32),
        compiler_params=params(8),
        name="pair_copies",
    )(mine, other)


def basis_kernel(count, sums_ref, high_ref, low_ref, basis_ref, squeezed_ref, square, out, out_sems):
    columns, width, quarter = basis_ref.shape
    bond = squeezed_ref.shape[1]

    def store(g):
        return pltpu.make_async_copy(out.at[g], basis_ref.at[:, pl.ds(pl.multiple_of(8 * g, 8), 8), :], out_sems.at[g])

    summed = jnp.sum(sums_ref[...], axis=0)
    flat = unfold([summed[i] for i in range(summed.shape[0])])
    square[...] = jnp.zeros_like(square)
    for i in range(columns // 8):
        square[8 * i:8 * i + 8, :columns] = flat[:, i * columns:(i + 1) * columns] / count
        first = columns * (columns // 8) + i * bond
        square[8 * i:8 * i + 8, columns:columns + bond] = flat[:, first:first + bond]
    matrix = square[...]
    wide = 8 * columns
    within = iota((columns, wide), 1) % (2 * columns)
    unit = (within // 8 * 4 + within % 4 == iota((columns, wide), 0)).astype(F32)
    row = iota((columns, LANES), 0)
    roots = jnp.zeros((columns, LANES), F32)
    block = 4
    for first in range(0, columns, block):
        cols = [jnp.broadcast_to(matrix[:, first + j:first + j + 1], (columns, LANES)) for j in range(block)]
        for j in range(block):
            k = first + j
            pivot = cols[j][k:k + 1]
            factor = jnp.where(row > k, cols[j] * (1.0 / pivot), 0.0)
            for i in range(j + 1, block):
                cols[i] = cols[i] - factor * cols[i][k:k + 1]
            matrix = matrix - factor * matrix[k:k + 1]
            unit = unit - jnp.concatenate([factor] * (wide // LANES), axis=1) * unit[k:k + 1]
            roots = jnp.where(row == k, 1.0 / jnp.sqrt(pivot), roots)
    squeezed_ref[...] = (matrix * roots)[:, columns:columns + bond] / count ** 0.5
    inverse = unit * jnp.concatenate([roots] * (wide // LANES), axis=1)
    spread = jnp.broadcast_to(inverse[:, None, :], (columns, 8, wide)).reshape(wide, wide)
    lane = iota((wide, wide), 1)
    same = lane // (2 * columns) * 2 + lane // 4 % 2 == iota((wide, wide), 0) % 8
    left_high, left_low = halves(jnp.where(same, spread, 0.0))

    def group(g, carry):
        high = high_ref[pl.ds(4 * g, 4)].reshape(wide, quarter)
        low = low_ref[pl.ds(4 * g, 4)].reshape(wide, quarter)
        result = jnp.dot(left_high, high, preferred_element_type=F32)
        result += jnp.dot(left_low, high, preferred_element_type=F32)
        result += jnp.dot(left_high, low, preferred_element_type=F32)
        out[g] = result.reshape(columns, 8, quarter)
        store(g).start()
        return carry

    lax.fori_loop(0, width // 8, group, 0)
    lax.fori_loop(0, width // 8, lambda g, carry: (store(g).wait(), carry)[1], 0)


def basis_of(sums, high, low, bond, count):
    pairs, doubled, quarter = high.shape
    width, columns = 2 * pairs, doubled // 2
    return pl.pallas_call(
        functools.partial(basis_kernel, float(count)),
        in_specs=[VMEM] * 3,
        out_specs=[HBM, VMEM],
        out_shape=[jax.ShapeDtypeStruct((columns, width, quarter), F32), jax.ShapeDtypeStruct((columns, bond), F32)],
        scratch_shapes=[
            pltpu.VMEM((columns, LANES), F32),
            pltpu.VMEM((width // 8, columns, 8, quarter), F32),
            pltpu.SemaphoreType.DMA((width // 8,)),
        ],
        cost_estimate=pl.CostEstimate(flops=2 * columns * columns * width * quarter * 24, bytes_accessed=4 * columns * width * quarter, transcendentals=0),
        compiler_params=params(16),
        name="basis_of",
    )(sums, high, low)


def per_device(factor_a, factor_b, next_factor, sketch_leg, sketch_rows):
    rows, cols = lax.axis_size("rows"), lax.axis_size("cols")
    devices = rows * cols
    local_rows, width, bond = factor_a.shape
    quarter = local_rows // cols
    count = local_rows * rows * width
    a = jnp.transpose(factor_a, (1, 2, 0))
    b = jnp.transpose(factor_b, (1, 2, 0)).reshape(width // 2, 2 * bond, local_rows)
    nxt = jnp.transpose(next_factor, (1, 2, 0))
    own = sketch_rows.shape[1]
    operands = [pltpu.with_memory_space_constraint(v, pltpu.HBM) for v in (sketch_rows.T, b, a)]
    partial, a_own = far_sum(*operands, quarter)
    each = -(-(width // 2) // rows)
    partial = jnp.pad(partial, ((0, each * rows - width // 2), (0, 0), (0, 0))).reshape(rows, each, own, LANES)
    parts = lax.all_to_all(partial, "rows", 0, 0)
    parities = [[i for i in range(devices) if i % 2 == parity] for parity in range(2)]
    pieces = lax.all_to_all(piece_copies(parts, devices // 2, bond), BOTH, 0, 0, axis_index_groups=parities)
    far_own = pieces.reshape(rows, cols // 2, each, own, LANES)
    swap = [(i, i ^ 1) for i in range(cols)]
    far_other = lax.ppermute(far_own, "cols", swap)
    near_high, near_low = near_sums(sketch_leg.T, a_own)
    high, low, sums = sketch_products(far_own, far_other, near_high, near_low, nxt)
    sums = pair_copies(sums, lax.ppermute(sums, "cols", swap), devices // 2)
    sums = lax.all_to_all(sums, BOTH, 0, 0, axis_index_groups=parities)
    basis, squeezed = basis_of(sums, high, low, bond, count)
    return jnp.transpose(basis, (0, 2, 1)), squeezed


def solution(mesh):
    return jax.shard_map(
        per_device,
        mesh=mesh,
        in_specs=(
            P("rows", None, None),
            P("rows", None, None),
            P(BOTH, None, None),
            P(),
            P("rows", "cols"),
        ),
        out_specs=(P(None, BOTH, None), P()),
        check_vma=False,
    )
```

```python
import functools

import jax
import jax.numpy as jnp
from jax import lax
from jax.experimental import pallas as pl
from jax.experimental.pallas import tpu as pltpu
from jax.sharding import PartitionSpec as P

BOTH = ("rows", "cols")
F32, BF16 = jnp.float32, jnp.bfloat16
LANES = 128
VMEM = pl.BlockSpec(memory_space=pltpu.VMEM)
HBM = pl.BlockSpec(memory_space=pltpu.HBM)
NT = (((1,), (1,)), ((), ()))


def iota(shape, axis):
    return lax.broadcasted_iota(jnp.int32, shape, axis)


def halves(value):
    high = value.astype(BF16)
    return high, (value - high.astype(F32)).astype(BF16)


def params(mib):
    return pltpu.CompilerParams(vmem_limit_bytes=mib << 20)


def far_kernel(rows_ref, b_ref, a_ref, out_ref, own_ref, rows_buf, buf, rows_sem, own_sem, sems):
    pairs, used, _ = b_ref.shape
    chunks = sems.shape[0]
    step = pairs // chunks
    quarter = own_ref.shape[2]
    start = pl.multiple_of(lax.axis_index("cols") * quarter, LANES)

    def fetch(c):
        part = pl.ds(c * step, step)
        return pltpu.make_async_copy(b_ref.at[part], buf.at[part], sems.at[c])

    rows_copy = pltpu.make_async_copy(rows_ref, rows_buf, rows_sem)
    rows_copy.start()
    ahead = 2
    for c in range(ahead):
        fetch(c).start()
    own_copy = pltpu.make_async_copy(a_ref.at[:, :, pl.ds(start, quarter)], own_ref, own_sem)
    own, lanes = out_ref.shape[1:]
    out_ref[:, :, used:] = jnp.zeros((pairs, own, lanes - used), F32)
    rows_copy.wait()
    for c in range(ahead, chunks):
        fetch(c).start()
    own_copy.start()
    for c in range(chunks):
        fetch(c).wait()
        for i in range(step):
            pair = c * step + i
            out_ref[pair, :, :used] = lax.dot_general(rows_buf[...], buf[pair], NT, preferred_element_type=F32)
    own_copy.wait()


def far_sum(rows_t, b_pairs, a_t, quarter):
    pairs, used, depth = b_pairs.shape
    chunks = pairs // 6
    own = rows_t.shape[0]
    return pl.pallas_call(
        far_kernel,
        in_specs=[HBM] * 3,
        out_specs=[VMEM] * 2,
        out_shape=[jax.ShapeDtypeStruct((pairs, own, LANES), F32), jax.ShapeDtypeStruct(a_t.shape[:2] + (quarter,), BF16)],
        scratch_shapes=[
            pltpu.VMEM(rows_t.shape, BF16),
            pltpu.VMEM((pairs, used, depth), BF16),
            pltpu.SemaphoreType.DMA,
            pltpu.SemaphoreType.DMA,
            pltpu.SemaphoreType.DMA((chunks,)),
        ],
        cost_estimate=pl.CostEstimate(flops=2 * own * pairs * used * depth, bytes_accessed=2 * pairs * used * depth, transcendentals=0),
        compiler_params=params(16),
        name="far_sum",
    )(rows_t, b_pairs, a_t)


def near_kernel(leg_ref, a_ref, high_ref, low_ref):
    columns, width = leg_ref.shape
    _, bond, quarter = high_ref.shape
    deep = 16
    wide = width * deep
    spread = (iota((width, wide), 1) // deep == iota((width, wide), 0)).astype(BF16)
    tiled = jnp.dot(leg_ref[...], spread, preferred_element_type=F32)
    tiled = jnp.broadcast_to(tiled[:, None, :], (columns, deep, wide)).reshape(columns * deep, wide)
    same = iota(tiled.shape, 1) % deep == iota(tiled.shape, 0) % deep
    weights = jnp.where(same, tiled, 0.0).astype(BF16)
    for first in range(0, bond, deep):
        part = a_ref[:, first:first + deep, :].reshape(wide, quarter)
        high, low = halves(jnp.dot(weights, part, preferred_element_type=F32))
        high_ref[:, first:first + deep, :] = high.reshape(columns, deep, quarter)
        low_ref[:, first:first + deep, :] = low.reshape(columns, deep, quarter)


def near_sums(leg_t, a_own):
    width, bond, quarter = a_own.shape
    columns = leg_t.shape[0]
    shape = jax.ShapeDtypeStruct((columns, bond, quarter), BF16)
    return pl.pallas_call(
        near_kernel,
        in_specs=[VMEM, VMEM],
        out_specs=[VMEM, VMEM],
        out_shape=[shape, shape],
        cost_estimate=pl.CostEstimate(flops=32 * columns * bond * width * quarter, bytes_accessed=2 * width * bond * quarter, transcendentals=0),
        compiler_params=params(16),
        name="near_sums",
    )(leg_t, a_own)


def piece_kernel(bond, parts_ref, out_ref):
    piece = jnp.sum(parts_ref[...], axis=0)
    half = piece.shape[1] // 2
    crossed = pltpu.roll(piece, half, 1)
    upper = iota(piece.shape, 1) < half
    left = iota(piece.shape, 2) < bond
    crossed = jnp.where(upper, pltpu.roll(crossed, bond, 2), pltpu.roll(crossed, LANES - bond, 2))
    piece = jnp.where(upper == left, piece, crossed)
    for i in range(out_ref.shape[0]):
        out_ref[i] = piece


def piece_copies(parts, copies, bond):
    return pl.pallas_call(
        functools.partial(piece_kernel, bond),
        in_specs=[VMEM],
        out_specs=VMEM,
        out_shape=jax.ShapeDtypeStruct((copies,) + parts.shape[1:], F32),
        compiler_params=params(8),
        name="piece_copies",
    )(parts)


def sketch_kernel(own_ref, other_ref, near_high_ref, near_low_ref, next_ref, high_ref, low_ref, sums_ref, sketch, wide_ref):
    groups, own = own_ref.shape[1], own_ref.shape[3]
    columns, bond, quarter = near_high_ref.shape
    pairs = sketch.shape[0]
    part = own // 2
    wide = part * bond
    parity = lax.axis_index("cols") % 2
    lane = iota((LANES, wide), 1) % bond
    keep = [(iota((LANES, wide), 0) == lane + half * bond).astype(BF16) for half in range(2)]
    same = iota((pairs * own, wide), 1) // bond == iota((pairs * own, wide), 0) % part

    def widen(far_ref, odd, g):
        far = halves(far_ref[:, g].reshape(-1, LANES)[:pairs * own])
        for half in range(2):
            block = 2 * (2 * g + odd) + half
            for i, piece in enumerate(far):
                value = jnp.dot(piece, keep[half], preferred_element_type=F32)
                wide_ref[block, pl.ds(i * pairs * own, pairs * own), :] = jnp.where(same, value, 0.0).astype(BF16)

    for g in range(groups):
        widen(own_ref, parity, g)
        widen(other_ref, 1 - parity, g)
    for block in range(columns // part):
        near_high = near_high_ref[block * part:(block + 1) * part].reshape(wide, quarter)
        near_low = near_low_ref[block * part:(block + 1) * part].reshape(wide, quarter)
        both = jnp.dot(wide_ref[block], near_high, preferred_element_type=F32)
        cross = jnp.dot(wide_ref[block, :pairs * own, :], near_low, preferred_element_type=F32)
        result = both[:pairs * own] + both[pairs * own:] + cross
        sketch[:, block * own:(block + 1) * own, :] = result.reshape(pairs, own, quarter)

    def products(i, total):
        for step in range(pairs // 2):
            pair = pairs // 2 * i + step
            high, low = halves(sketch[pair])
            high_ref[pair] = high
            low_ref[pair] = low
            left = jnp.concatenate([high, next_ref[2 * pair], next_ref[2 * pair + 1]], axis=0)
            total = total + lax.dot_general(left, jnp.concatenate([high, low], axis=0), NT, preferred_element_type=F32)
        return total

    doubled = 2 * columns
    rows = doubled + 2 * bond
    total = lax.fori_loop(0, 2, products, jnp.zeros((rows, LANES), F32))
    row, lane = iota((rows, LANES), 0), iota((rows, LANES), 1)
    row_y = jnp.where(row < doubled, row // part % 2, (row >= doubled + bond).astype(jnp.int32))
    total = jnp.where(row_y == lane // part % 2, total, 0.0)
    lane, target = iota((LANES, doubled), 0), iota((LANES, doubled), 1)
    column = lane % doubled // own * part + lane % part
    pick = (column == target % columns) & ((target < columns) | (lane >= doubled))
    packed = jnp.dot(total, pick.astype(F32), preferred_element_type=F32, precision=lax.Precision.HIGHEST)
    squares = packed[:doubled].reshape(doubled // own, own, doubled)
    squares = squares + pltpu.roll(squares, part, 1)
    upper = iota((own, doubled), 0) < part
    squares = jnp.concatenate([jnp.where(upper, squares[2 * i], squares[2 * i + 1]) for i in range(columns // own)], axis=0)
    squeezes = packed[doubled:doubled + bond] + packed[doubled + bond:]
    padded = jnp.concatenate([squares, squeezes, jnp.zeros((LANES - columns - bond, doubled), F32)], axis=0)
    padded = jnp.concatenate([padded, jnp.zeros((LANES, LANES - doubled), F32)], axis=1)
    turned = padded.T
    gram = squares[:, :columns] + turned[columns:doubled, :columns]
    squeeze = turned[:columns, columns:columns + bond]
    flat = jnp.concatenate([v[8 * i:8 * i + 8] for v in (gram, squeeze) for i in range(columns // 8)], axis=1)
    blocks = fold(flat)
    for i, block in enumerate(blocks):
        sums_ref[i] = block


def fold(flat):
    blocks = []
    whole = flat.shape[1] // LANES * LANES
    for i in range(0, whole, LANES):
        blocks += [flat[:4, i:i + LANES], flat[4:, i:i + LANES]]
    if whole < flat.shape[1]:
        blocks.append(jnp.concatenate([flat[:4, whole:], flat[4:, whole:]], axis=1))
    return blocks


def unfold(blocks):
    flat = [jnp.concatenate(blocks[i:i + 2], axis=0) for i in range(0, len(blocks) - 1, 2)]
    if len(blocks) % 2:
        last = blocks[-1]
        flat.append(jnp.concatenate([last[:, :LANES // 2], last[:, LANES // 2:]], axis=0))
    return jnp.concatenate(flat, axis=1)


def sketch_products(far_own, far_other, near_high, near_low, nxt):
    columns, bond, quarter = near_high.shape
    width, own = nxt.shape[0], far_own.shape[3]
    shape = jax.ShapeDtypeStruct((width // 2, 2 * columns, quarter), BF16)
    blocks = columns * (columns + bond) // 512
    return pl.pallas_call(
        sketch_kernel,
        in_specs=[VMEM] * 5,
        out_specs=[VMEM] * 3,
        out_shape=[shape, shape, jax.ShapeDtypeStruct((blocks, 4, LANES), F32)],
        scratch_shapes=[
            pltpu.VMEM((width // 2, 2 * columns, quarter), F32),
            pltpu.VMEM((2 * columns // own, own * width, own // 2 * bond), BF16),
        ],
        cost_estimate=pl.CostEstimate(flops=2 * columns * bond * width * quarter * 24, bytes_accessed=8 * columns * width * quarter, transcendentals=0),
        compiler_params=params(16),
        name="sketch_products",
    )(far_own, far_other, near_high, near_low, nxt)


def pair_kernel(mine_ref, other_ref, out_ref):
    both = mine_ref[...] + other_ref[...]
    for i in range(out_ref.shape[0]):
        out_ref[i] = both


def pair_copies(mine, other, copies):
    return pl.pallas_call(
        pair_kernel,
        in_specs=[VMEM] * 2,
        out_specs=VMEM,
        out_shape=jax.ShapeDtypeStruct((copies,) + mine.shape, F32),
        compiler_params=params(8),
        name="pair_copies",
    )(mine, other)


def basis_kernel(count, sums_ref, high_ref, low_ref, basis_ref, squeezed_ref, square, out, out_sems):
    columns, width, quarter = basis_ref.shape
    bond = squeezed_ref.shape[1]

    def store(g):
        return pltpu.make_async_copy(out.at[g], basis_ref.at[:, pl.ds(pl.multiple_of(8 * g, 8), 8), :], out_sems.at[g])

    summed = jnp.sum(sums_ref[...], axis=0)
    flat = unfold([summed[i] for i in range(summed.shape[0])])
    square[...] = jnp.zeros_like(square)
    for i in range(columns // 8):
        square[8 * i:8 * i + 8, :columns] = flat[:, i * columns:(i + 1) * columns] / count
        first = columns * (columns // 8) + i * bond
        square[8 * i:8 * i + 8, columns:columns + bond] = flat[:, first:first + bond]
    matrix = square[...]
    wide = 8 * columns
    within = iota((columns, wide), 1) % (2 * columns)
    unit = (within // 8 * 4 + within % 4 == iota((columns, wide), 0)).astype(F32)
    row = iota((columns, LANES), 0)
    roots = jnp.zeros((columns, LANES), F32)
    block = 4
    for first in range(0, columns, block):
        cols = [jnp.broadcast_to(matrix[:, first + j:first + j + 1], (columns, LANES)) for j in range(block)]
        for j in range(block):
            k = first + j
            pivot = cols[j][k:k + 1]
            factor = jnp.where(row > k, cols[j] * (1.0 / pivot), 0.0)
            for i in range(j + 1, block):
                cols[i] = cols[i] - factor * cols[i][k:k + 1]
            matrix = matrix - factor * matrix[k:k + 1]
            unit = unit - jnp.concatenate([factor] * (wide // LANES), axis=1) * unit[k:k + 1]
            roots = jnp.where(row == k, 1.0 / jnp.sqrt(pivot), roots)
    squeezed_ref[...] = (matrix * roots)[:, columns:columns + bond] / count ** 0.5
    inverse = unit * jnp.concatenate([roots] * (wide // LANES), axis=1)
    spread = jnp.broadcast_to(inverse[:, None, :], (columns, 8, wide)).reshape(wide, wide)
    lane = iota((wide, wide), 1)
    same = lane // (2 * columns) * 2 + lane // 4 % 2 == iota((wide, wide), 0) % 8
    left_high, left_low = halves(jnp.where(same, spread, 0.0))

    def group(g, carry):
        high = high_ref[pl.ds(4 * g, 4)].reshape(wide, quarter)
        low = low_ref[pl.ds(4 * g, 4)].reshape(wide, quarter)
        result = jnp.dot(left_high, high, preferred_element_type=F32)
        result += jnp.dot(left_low, high, preferred_element_type=F32)
        result += jnp.dot(left_high, low, preferred_element_type=F32)
        out[g] = result.reshape(columns, 8, quarter)
        store(g).start()
        return carry

    lax.fori_loop(0, width // 8, group, 0, unroll=True)
    lax.fori_loop(0, width // 8, lambda g, carry: (store(g).wait(), carry)[1], 0)


def basis_of(sums, high, low, bond, count):
    pairs, doubled, quarter = high.shape
    width, columns = 2 * pairs, doubled // 2
    return pl.pallas_call(
        functools.partial(basis_kernel, float(count)),
        in_specs=[VMEM] * 3,
        out_specs=[HBM, VMEM],
        out_shape=[jax.ShapeDtypeStruct((columns, width, quarter), F32), jax.ShapeDtypeStruct((columns, bond), F32)],
        scratch_shapes=[
            pltpu.VMEM((columns, LANES), F32),
            pltpu.VMEM((width // 8, columns, 8, quarter), F32),
            pltpu.SemaphoreType.DMA((width // 8,)),
        ],
        cost_estimate=pl.CostEstimate(flops=2 * columns * columns * width * quarter * 24, bytes_accessed=4 * columns * width * quarter, transcendentals=0),
        compiler_params=params(16),
        name="basis_of",
    )(sums, high, low)


def per_device(factor_a, factor_b, next_factor, sketch_leg, sketch_rows):
    rows, cols = lax.axis_size("rows"), lax.axis_size("cols")
    devices = rows * cols
    local_rows, width, bond = factor_a.shape
    quarter = local_rows // cols
    count = local_rows * rows * width
    a = jnp.transpose(factor_a, (1, 2, 0))
    b = jnp.transpose(factor_b, (1, 2, 0)).reshape(width // 2, 2 * bond, local_rows)
    nxt = jnp.transpose(next_factor, (1, 2, 0))
    own = sketch_rows.shape[1]
    operands = [pltpu.with_memory_space_constraint(v, pltpu.HBM) for v in (sketch_rows.T, b, a)]
    partial, a_own = far_sum(*operands, quarter)
    each = -(-(width // 2) // rows)
    partial = jnp.pad(partial, ((0, each * rows - width // 2), (0, 0), (0, 0))).reshape(rows, each, own, LANES)
    parts = lax.all_to_all(partial, "rows", 0, 0)
    parities = [[i for i in range(devices) if i % 2 == parity] for parity in range(2)]
    pieces = lax.all_to_all(piece_copies(parts, devices // 2, bond), BOTH, 0, 0, axis_index_groups=parities)
    far_own = pieces.reshape(rows, cols // 2, each, own, LANES)
    swap = [(i, i ^ 1) for i in range(cols)]
    far_other = lax.ppermute(far_own, "cols", swap)
    near_high, near_low = near_sums(sketch_leg.T, a_own)
    high, low, sums = sketch_products(far_own, far_other, near_high, near_low, nxt)
    sums = pair_copies(sums, lax.ppermute(sums, "cols", swap), devices // 2)
    sums = lax.all_to_all(sums, BOTH, 0, 0, axis_index_groups=parities)
    basis, squeezed = basis_of(sums, high, low, bond, count)
    return jnp.transpose(basis, (0, 2, 1)), squeezed


def solution(mesh):
    return jax.shard_map(
        per_device,
        mesh=mesh,
        in_specs=(
            P("rows", None, None),
            P("rows", None, None),
            P(BOTH, None, None),
            P(),
            P("rows", "cols"),
        ),
        out_specs=(P(None, BOTH, None), P()),
        check_vma=False,
    )
```

```python
import functools

import jax
import jax.numpy as jnp
from jax import lax
from jax.experimental import pallas as pl
from jax.experimental.pallas import tpu as pltpu
from jax.sharding import PartitionSpec as P

BOTH = ("rows", "cols")
F32, BF16 = jnp.float32, jnp.bfloat16
LANES = 128
VMEM = pl.BlockSpec(memory_space=pltpu.VMEM)
HBM = pl.BlockSpec(memory_space=pltpu.HBM)
NT = (((1,), (1,)), ((), ()))


def iota(shape, axis):
    return lax.broadcasted_iota(jnp.int32, shape, axis)


def halves(value):
    high = value.astype(BF16)
    return high, (value - high.astype(F32)).astype(BF16)


def params(mib):
    return pltpu.CompilerParams(vmem_limit_bytes=mib << 20)


def far_kernel(rows_ref, b_ref, a_ref, out_ref, own_ref, rows_buf, buf, rows_sem, own_sem, sems):
    pairs, used, _ = b_ref.shape
    chunks = sems.shape[0]
    step = pairs // chunks
    quarter = own_ref.shape[2]
    start = pl.multiple_of(lax.axis_index("cols") * quarter, LANES)

    def fetch(c):
        part = pl.ds(c * step, step)
        return pltpu.make_async_copy(b_ref.at[part], buf.at[part], sems.at[c])

    rows_copy = pltpu.make_async_copy(rows_ref, rows_buf, rows_sem)
    rows_copy.start()
    ahead = 2
    for c in range(ahead):
        fetch(c).start()
    own_copy = pltpu.make_async_copy(a_ref.at[:, :, pl.ds(start, quarter)], own_ref, own_sem)
    own, lanes = out_ref.shape[1:]
    out_ref[:, :, used:] = jnp.zeros((pairs, own, lanes - used), F32)
    rows_copy.wait()
    for c in range(ahead, chunks):
        fetch(c).start()
    own_copy.start()
    for c in range(chunks):
        fetch(c).wait()
        for i in range(step):
            pair = c * step + i
            out_ref[pair, :, :used] = lax.dot_general(rows_buf[...], buf[pair], NT, preferred_element_type=F32)
    own_copy.wait()


def far_sum(rows_t, b_pairs, a_t, quarter):
    pairs, used, depth = b_pairs.shape
    chunks = pairs // 6
    own = rows_t.shape[0]
    return pl.pallas_call(
        far_kernel,
        in_specs=[HBM] * 3,
        out_specs=[VMEM] * 2,
        out_shape=[jax.ShapeDtypeStruct((pairs, own, LANES), F32), jax.ShapeDtypeStruct(a_t.shape[:2] + (quarter,), BF16)],
        scratch_shapes=[
            pltpu.VMEM(rows_t.shape, BF16),
            pltpu.VMEM((pairs, used, depth), BF16),
            pltpu.SemaphoreType.DMA,
            pltpu.SemaphoreType.DMA,
            pltpu.SemaphoreType.DMA((chunks,)),
        ],
        cost_estimate=pl.CostEstimate(flops=2 * own * pairs * used * depth, bytes_accessed=2 * pairs * used * depth, transcendentals=0),
        compiler_params=params(16),
        name="far_sum",
    )(rows_t, b_pairs, a_t)


def near_kernel(leg_ref, a_ref, high_ref, low_ref):
    columns, width = leg_ref.shape
    _, bond, quarter = high_ref.shape
    deep = 16
    wide = width * deep
    spread = (iota((width, wide), 1) // deep == iota((width, wide), 0)).astype(BF16)
    tiled = jnp.dot(leg_ref[...], spread, preferred_element_type=F32)
    tiled = jnp.broadcast_to(tiled[:, None, :], (columns, deep, wide)).reshape(columns * deep, wide)
    same = iota(tiled.shape, 1) % deep == iota(tiled.shape, 0) % deep
    weights = jnp.where(same, tiled, 0.0).astype(BF16)
    for first in range(0, bond, deep):
        part = a_ref[:, first:first + deep, :].reshape(wide, quarter)
        high, low = halves(jnp.dot(weights, part, preferred_element_type=F32))
        high_ref[:, first:first + deep, :] = high.reshape(columns, deep, quarter)
        low_ref[:, first:first + deep, :] = low.reshape(columns, deep, quarter)


def near_sums(leg_t, a_own):
    width, bond, quarter = a_own.shape
    columns = leg_t.shape[0]
    shape = jax.ShapeDtypeStruct((columns, bond, quarter), BF16)
    return pl.pallas_call(
        near_kernel,
        in_specs=[VMEM, VMEM],
        out_specs=[VMEM, VMEM],
        out_shape=[shape, shape],
        cost_estimate=pl.CostEstimate(flops=32 * columns * bond * width * quarter, bytes_accessed=2 * width * bond * quarter, transcendentals=0),
        compiler_params=params(16),
        name="near_sums",
    )(leg_t, a_own)


def piece_kernel(bond, parts_ref, out_ref):
    piece = jnp.sum(parts_ref[...], axis=0)
    half = piece.shape[1] // 2
    crossed = pltpu.roll(piece, half, 1)
    upper = iota(piece.shape, 1) < half
    left = iota(piece.shape, 2) < bond
    crossed = jnp.where(upper, pltpu.roll(crossed, bond, 2), pltpu.roll(crossed, LANES - bond, 2))
    piece = jnp.where(upper == left, piece, crossed)
    for i in range(out_ref.shape[0]):
        out_ref[i] = piece


def piece_copies(parts, copies, bond):
    return pl.pallas_call(
        functools.partial(piece_kernel, bond),
        in_specs=[VMEM],
        out_specs=VMEM,
        out_shape=jax.ShapeDtypeStruct((copies,) + parts.shape[1:], F32),
        compiler_params=params(8),
        name="piece_copies",
    )(parts)


def sketch_kernel(own_ref, other_ref, near_high_ref, near_low_ref, next_ref, high_ref, low_ref, sums_ref, sketch, wide_ref):
    groups, own = own_ref.shape[1], own_ref.shape[3]
    columns, bond, quarter = near_high_ref.shape
    pairs = sketch.shape[0]
    part = own // 2
    wide = part * bond
    parity = lax.axis_index("cols") % 2
    lane = iota((LANES, wide), 1) % bond
    keep = [(iota((LANES, wide), 0) == lane + half * bond).astype(BF16) for half in range(2)]
    same = iota((pairs * own, wide), 1) // bond == iota((pairs * own, wide), 0) % part

    def widen(far_ref, odd, g):
        far = halves(far_ref[:, g].reshape(-1, LANES)[:pairs * own])
        for half in range(2):
            block = 2 * (2 * g + odd) + half
            for i, piece in enumerate(far):
                value = jnp.dot(piece, keep[half], preferred_element_type=F32)
                wide_ref[block, pl.ds(i * pairs * own, pairs * own), :] = jnp.where(same, value, 0.0).astype(BF16)

    for g in range(groups):
        widen(own_ref, parity, g)
        widen(other_ref, 1 - parity, g)
    for block in range(columns // part):
        near_high = near_high_ref[block * part:(block + 1) * part].reshape(wide, quarter)
        near_low = near_low_ref[block * part:(block + 1) * part].reshape(wide, quarter)
        both = jnp.dot(wide_ref[block], near_high, preferred_element_type=F32)
        cross = jnp.dot(wide_ref[block, :pairs * own, :], near_low, preferred_element_type=F32)
        result = both[:pairs * own] + both[pairs * own:] + cross
        sketch[:, block * own:(block + 1) * own, :] = result.reshape(pairs, own, quarter)

    def products(i, total):
        for step in range(pairs // 2):
            pair = pairs // 2 * i + step
            high, low = halves(sketch[pair])
            high_ref[pair] = high
            low_ref[pair] = low
            left = jnp.concatenate([high, next_ref[2 * pair], next_ref[2 * pair + 1]], axis=0)
            total = total + lax.dot_general(left, jnp.concatenate([high, low], axis=0), NT, preferred_element_type=F32)
        return total

    doubled = 2 * columns
    rows = doubled + 2 * bond
    total = lax.fori_loop(0, 2, products, jnp.zeros((rows, LANES), F32))
    row, lane = iota((rows, LANES), 0), iota((rows, LANES), 1)
    row_y = jnp.where(row < doubled, row // part % 2, (row >= doubled + bond).astype(jnp.int32))
    total = jnp.where(row_y == lane // part % 2, total, 0.0)
    lane, target = iota((LANES, doubled), 0), iota((LANES, doubled), 1)
    column = lane % doubled // own * part + lane % part
    pick = (column == target % columns) & ((target < columns) | (lane >= doubled))
    packed = jnp.dot(total, pick.astype(F32), preferred_element_type=F32, precision=lax.Precision.HIGHEST)
    squares = packed[:doubled].reshape(doubled // own, own, doubled)
    squares = squares + pltpu.roll(squares, part, 1)
    upper = iota((own, doubled), 0) < part
    squares = jnp.concatenate([jnp.where(upper, squares[2 * i], squares[2 * i + 1]) for i in range(columns // own)], axis=0)
    squeezes = packed[doubled:doubled + bond] + packed[doubled + bond:]
    padded = jnp.concatenate([squares, squeezes, jnp.zeros((LANES - columns - bond, doubled), F32)], axis=0)
    padded = jnp.concatenate([padded, jnp.zeros((LANES, LANES - doubled), F32)], axis=1)
    turned = padded.T
    gram = squares[:, :columns] + turned[columns:doubled, :columns]
    squeeze = turned[:columns, columns:columns + bond]
    flat = jnp.concatenate([v[8 * i:8 * i + 8] for v in (gram, squeeze) for i in range(columns // 8)], axis=1)
    blocks = fold(flat)
    for i, block in enumerate(blocks):
        sums_ref[i] = block


def fold(flat):
    blocks = []
    whole = flat.shape[1] // LANES * LANES
    for i in range(0, whole, LANES):
        blocks += [flat[:4, i:i + LANES], flat[4:, i:i + LANES]]
    if whole < flat.shape[1]:
        blocks.append(jnp.concatenate([flat[:4, whole:], flat[4:, whole:]], axis=1))
    return blocks


def unfold(blocks):
    flat = [jnp.concatenate(blocks[i:i + 2], axis=0) for i in range(0, len(blocks) - 1, 2)]
    if len(blocks) % 2:
        last = blocks[-1]
        flat.append(jnp.concatenate([last[:, :LANES // 2], last[:, LANES // 2:]], axis=0))
    return jnp.concatenate(flat, axis=1)


def sketch_products(far_own, far_other, near_high, near_low, nxt):
    columns, bond, quarter = near_high.shape
    width, own = nxt.shape[0], far_own.shape[3]
    shape = jax.ShapeDtypeStruct((width // 2, 2 * columns, quarter), BF16)
    blocks = columns * (columns + bond) // 512
    return pl.pallas_call(
        sketch_kernel,
        in_specs=[VMEM] * 5,
        out_specs=[VMEM] * 3,
        out_shape=[shape, shape, jax.ShapeDtypeStruct((blocks, 4, LANES), F32)],
        scratch_shapes=[
            pltpu.VMEM((width // 2, 2 * columns, quarter), F32),
            pltpu.VMEM((2 * columns // own, own * width, own // 2 * bond), BF16),
        ],
        cost_estimate=pl.CostEstimate(flops=2 * columns * bond * width * quarter * 24, bytes_accessed=8 * columns * width * quarter, transcendentals=0),
        compiler_params=params(16),
        name="sketch_products",
    )(far_own, far_other, near_high, near_low, nxt)


def pair_kernel(mine_ref, other_ref, out_ref):
    both = mine_ref[...] + other_ref[...]
    for i in range(out_ref.shape[0]):
        out_ref[i] = both


def pair_copies(mine, other, copies):
    return pl.pallas_call(
        pair_kernel,
        in_specs=[VMEM] * 2,
        out_specs=VMEM,
        out_shape=jax.ShapeDtypeStruct((copies,) + mine.shape, F32),
        compiler_params=params(8),
        name="pair_copies",
    )(mine, other)


def basis_kernel(count, sums_ref, high_ref, low_ref, basis_ref, squeezed_ref, square, out, out_sems):
    columns, width, quarter = basis_ref.shape
    bond = squeezed_ref.shape[1]

    def store(g):
        return pltpu.make_async_copy(out.at[g], basis_ref.at[:, pl.ds(pl.multiple_of(8 * g, 8), 8), :], out_sems.at[g])

    summed = jnp.sum(sums_ref[...], axis=0)
    flat = unfold([summed[i] for i in range(summed.shape[0])])
    square[...] = jnp.zeros_like(square)
    for i in range(columns // 8):
        square[8 * i:8 * i + 8, :columns] = flat[:, i * columns:(i + 1) * columns] / count
        first = columns * (columns // 8) + i * bond
        square[8 * i:8 * i + 8, columns:columns + bond] = flat[:, first:first + bond]
    matrix = square[...]
    wide = 8 * columns
    within = iota((columns, wide), 1) % (2 * columns)
    unit = (within // 8 * 4 + within % 4 == iota((columns, wide), 0)).astype(F32)
    row = iota((columns, LANES), 0)
    roots = jnp.zeros((columns, LANES), F32)
    block = 16
    for first in range(0, columns, block):
        cols = [jnp.broadcast_to(matrix[:, first + j:first + j + 1], (columns, LANES)) for j in range(block)]
        for j in range(block):
            k = first + j
            pivot = cols[j][k:k + 1]
            factor = jnp.where(row > k, cols[j] * (1.0 / pivot), 0.0)
            for i in range(j + 1, block):
                cols[i] = cols[i] - factor * cols[i][k:k + 1]
            matrix = matrix - factor * matrix[k:k + 1]
            unit = unit - jnp.concatenate([factor] * (wide // LANES), axis=1) * unit[k:k + 1]
            roots = jnp.where(row == k, 1.0 / jnp.sqrt(pivot), roots)
    squeezed_ref[...] = (matrix * roots)[:, columns:columns + bond] / count ** 0.5
    inverse = unit * jnp.concatenate([roots] * (wide // LANES), axis=1)
    spread = jnp.broadcast_to(inverse[:, None, :], (columns, 8, wide)).reshape(wide, wide)
    lane = iota((wide, wide), 1)
    same = lane // (2 * columns) * 2 + lane // 4 % 2 == iota((wide, wide), 0) % 8
    left_high, left_low = halves(jnp.where(same, spread, 0.0))

    def group(g, carry):
        high = high_ref[pl.ds(4 * g, 4)].reshape(wide, quarter)
        low = low_ref[pl.ds(4 * g, 4)].reshape(wide, quarter)
        result = jnp.dot(left_high, high, preferred_element_type=F32)
        result += jnp.dot(left_low, high, preferred_element_type=F32)
        result += jnp.dot(left_high, low, preferred_element_type=F32)
        out[g] = result.reshape(columns, 8, quarter)
        store(g).start()
        return carry

    lax.fori_loop(0, width // 8, group, 0, unroll=True)
    lax.fori_loop(0, width // 8, lambda g, carry: (store(g).wait(), carry)[1], 0)


def basis_of(sums, high, low, bond, count):
    pairs, doubled, quarter = high.shape
    width, columns = 2 * pairs, doubled // 2
    return pl.pallas_call(
        functools.partial(basis_kernel, float(count)),
        in_specs=[VMEM] * 3,
        out_specs=[HBM, VMEM],
        out_shape=[jax.ShapeDtypeStruct((columns, width, quarter), F32), jax.ShapeDtypeStruct((columns, bond), F32)],
        scratch_shapes=[
            pltpu.VMEM((columns, LANES), F32),
            pltpu.VMEM((width // 8, columns, 8, quarter), F32),
            pltpu.SemaphoreType.DMA((width // 8,)),
        ],
        cost_estimate=pl.CostEstimate(flops=2 * columns * columns * width * quarter * 24, bytes_accessed=4 * columns * width * quarter, transcendentals=0),
        compiler_params=params(16),
        name="basis_of",
    )(sums, high, low)


def per_device(factor_a, factor_b, next_factor, sketch_leg, sketch_rows):
    rows, cols = lax.axis_size("rows"), lax.axis_size("cols")
    devices = rows * cols
    local_rows, width, bond = factor_a.shape
    quarter = local_rows // cols
    count = local_rows * rows * width
    a = jnp.transpose(factor_a, (1, 2, 0))
    b = jnp.transpose(factor_b, (1, 2, 0)).reshape(width // 2, 2 * bond, local_rows)
    nxt = jnp.transpose(next_factor, (1, 2, 0))
    own = sketch_rows.shape[1]
    operands = [pltpu.with_memory_space_constraint(v, pltpu.HBM) for v in (sketch_rows.T, b, a)]
    partial, a_own = far_sum(*operands, quarter)
    each = -(-(width // 2) // rows)
    partial = jnp.pad(partial, ((0, each * rows - width // 2), (0, 0), (0, 0))).reshape(rows, each, own, LANES)
    parts = lax.all_to_all(partial, "rows", 0, 0)
    parities = [[i for i in range(devices) if i % 2 == parity] for parity in range(2)]
    pieces = lax.all_to_all(piece_copies(parts, devices // 2, bond), BOTH, 0, 0, axis_index_groups=parities)
    far_own = pieces.reshape(rows, cols // 2, each, own, LANES)
    swap = [(i, i ^ 1) for i in range(cols)]
    far_other = lax.ppermute(far_own, "cols", swap)
    near_high, near_low = near_sums(sketch_leg.T, a_own)
    high, low, sums = sketch_products(far_own, far_other, near_high, near_low, nxt)
    sums = pair_copies(sums, lax.ppermute(sums, "cols", swap), devices // 2)
    sums = lax.all_to_all(sums, BOTH, 0, 0, axis_index_groups=parities)
    basis, squeezed = basis_of(sums, high, low, bond, count)
    return jnp.transpose(basis, (0, 2, 1)), squeezed


def solution(mesh):
    return jax.shard_map(
        per_device,
        mesh=mesh,
        in_specs=(
            P("rows", None, None),
            P("rows", None, None),
            P(BOTH, None, None),
            P(),
            P("rows", "cols"),
        ),
        out_specs=(P(None, BOTH, None), P()),
        check_vma=False,
    )
```

```python
import functools

import jax
import jax.numpy as jnp
from jax import lax
from jax.experimental import pallas as pl
from jax.experimental.pallas import tpu as pltpu
from jax.sharding import PartitionSpec as P

BOTH = ("rows", "cols")
F32, BF16 = jnp.float32, jnp.bfloat16
LANES = 128
VMEM = pl.BlockSpec(memory_space=pltpu.VMEM)
HBM = pl.BlockSpec(memory_space=pltpu.HBM)
NT = (((1,), (1,)), ((), ()))


def iota(shape, axis):
    return lax.broadcasted_iota(jnp.int32, shape, axis)


def halves(value):
    high = value.astype(BF16)
    return high, (value - high.astype(F32)).astype(BF16)


def params(mib):
    return pltpu.CompilerParams(vmem_limit_bytes=mib << 20)


def far_kernel(rows_ref, b_ref, a_ref, out_ref, own_ref, rows_buf, buf, rows_sem, own_sem, sems):
    pairs, used, _ = b_ref.shape
    chunks = sems.shape[0]
    step = pairs // chunks
    quarter = own_ref.shape[2]
    start = pl.multiple_of(lax.axis_index("cols") * quarter, LANES)

    def fetch(c):
        part = pl.ds(c * step, step)
        return pltpu.make_async_copy(b_ref.at[part], buf.at[part], sems.at[c])

    rows_copy = pltpu.make_async_copy(rows_ref, rows_buf, rows_sem)
    rows_copy.start()
    ahead = 2
    for c in range(ahead):
        fetch(c).start()
    own_copy = pltpu.make_async_copy(a_ref.at[:, :, pl.ds(start, quarter)], own_ref, own_sem)
    own, lanes = out_ref.shape[1:]
    out_ref[:, :, used:] = jnp.zeros((pairs, own, lanes - used), F32)
    rows_copy.wait()
    for c in range(ahead, chunks):
        fetch(c).start()
    own_copy.start()
    for c in range(chunks):
        fetch(c).wait()
        for i in range(step):
            pair = c * step + i
            out_ref[pair, :, :used] = lax.dot_general(rows_buf[...], buf[pair], NT, preferred_element_type=F32)
    own_copy.wait()


def far_sum(rows_t, b_pairs, a_t, quarter):
    pairs, used, depth = b_pairs.shape
    chunks = pairs // 6
    own = rows_t.shape[0]
    return pl.pallas_call(
        far_kernel,
        in_specs=[HBM] * 3,
        out_specs=[VMEM] * 2,
        out_shape=[jax.ShapeDtypeStruct((pairs, own, LANES), F32), jax.ShapeDtypeStruct(a_t.shape[:2] + (quarter,), BF16)],
        scratch_shapes=[
            pltpu.VMEM(rows_t.shape, BF16),
            pltpu.VMEM((pairs, used, depth), BF16),
            pltpu.SemaphoreType.DMA,
            pltpu.SemaphoreType.DMA,
            pltpu.SemaphoreType.DMA((chunks,)),
        ],
        cost_estimate=pl.CostEstimate(flops=2 * own * pairs * used * depth, bytes_accessed=2 * pairs * used * depth, transcendentals=0),
        compiler_params=params(16),
        name="far_sum",
    )(rows_t, b_pairs, a_t)


def near_kernel(leg_ref, a_ref, high_ref, low_ref):
    columns, width = leg_ref.shape
    _, bond, quarter = high_ref.shape
    deep = 16
    wide = width * deep
    spread = (iota((width, wide), 1) // deep == iota((width, wide), 0)).astype(BF16)
    tiled = jnp.dot(leg_ref[...], spread, preferred_element_type=F32)
    tiled = jnp.broadcast_to(tiled[:, None, :], (columns, deep, wide)).reshape(columns * deep, wide)
    same = iota(tiled.shape, 1) % deep == iota(tiled.shape, 0) % deep
    weights = jnp.where(same, tiled, 0.0).astype(BF16)
    for first in range(0, bond, deep):
        part = a_ref[:, first:first + deep, :].reshape(wide, quarter)
        high, low = halves(jnp.dot(weights, part, preferred_element_type=F32))
        high_ref[:, first:first + deep, :] = high.reshape(columns, deep, quarter)
        low_ref[:, first:first + deep, :] = low.reshape(columns, deep, quarter)


def near_sums(leg_t, a_own):
    width, bond, quarter = a_own.shape
    columns = leg_t.shape[0]
    shape = jax.ShapeDtypeStruct((columns, bond, quarter), BF16)
    return pl.pallas_call(
        near_kernel,
        in_specs=[VMEM, VMEM],
        out_specs=[VMEM, VMEM],
        out_shape=[shape, shape],
        cost_estimate=pl.CostEstimate(flops=32 * columns * bond * width * quarter, bytes_accessed=2 * width * bond * quarter, transcendentals=0),
        compiler_params=params(16),
        name="near_sums",
    )(leg_t, a_own)


def piece_kernel(bond, parts_ref, out_ref):
    piece = jnp.sum(parts_ref[...], axis=0)
    half = piece.shape[1] // 2
    crossed = pltpu.roll(piece, half, 1)
    upper = iota(piece.shape, 1) < half
    left = iota(piece.shape, 2) < bond
    crossed = jnp.where(upper, pltpu.roll(crossed, bond, 2), pltpu.roll(crossed, LANES - bond, 2))
    piece = jnp.where(upper == left, piece, crossed)
    for i in range(out_ref.shape[0]):
        out_ref[i] = piece


def piece_copies(parts, copies, bond):
    return pl.pallas_call(
        functools.partial(piece_kernel, bond),
        in_specs=[VMEM],
        out_specs=VMEM,
        out_shape=jax.ShapeDtypeStruct((copies,) + parts.shape[1:], F32),
        compiler_params=params(8),
        name="piece_copies",
    )(parts)


def sketch_kernel(own_ref, other_ref, near_high_ref, near_low_ref, next_ref, high_ref, low_ref, sums_ref, sketch, wide_ref):
    groups, own = own_ref.shape[1], own_ref.shape[3]
    columns, bond, quarter = near_high_ref.shape
    pairs = sketch.shape[0]
    part = own // 2
    wide = part * bond
    parity = lax.axis_index("cols") % 2
    lane = iota((LANES, wide), 1) % bond
    keep = [(iota((LANES, wide), 0) == lane + half * bond).astype(BF16) for half in range(2)]
    same = iota((pairs * own, wide), 1) // bond == iota((pairs * own, wide), 0) % part

    def widen(far_ref, odd, g):
        far = halves(far_ref[:, g].reshape(-1, LANES)[:pairs * own])
        for half in range(2):
            block = 2 * (2 * g + odd) + half
            for i, piece in enumerate(far):
                value = jnp.dot(piece, keep[half], preferred_element_type=F32)
                wide_ref[block, pl.ds(i * pairs * own, pairs * own), :] = jnp.where(same, value, 0.0).astype(BF16)

    for g in range(groups):
        widen(own_ref, parity, g)
        widen(other_ref, 1 - parity, g)
    for block in range(columns // part):
        near_high = near_high_ref[block * part:(block + 1) * part].reshape(wide, quarter)
        near_low = near_low_ref[block * part:(block + 1) * part].reshape(wide, quarter)
        both = jnp.dot(wide_ref[block], near_high, preferred_element_type=F32)
        cross = jnp.dot(wide_ref[block, :pairs * own, :], near_low, preferred_element_type=F32)
        result = both[:pairs * own] + both[pairs * own:] + cross
        sketch[:, block * own:(block + 1) * own, :] = result.reshape(pairs, own, quarter)

    def products(i, total):
        for step in range(pairs // 2):
            pair = pairs // 2 * i + step
            high, low = halves(sketch[pair])
            high_ref[pair] = high
            low_ref[pair] = low
            left = jnp.concatenate([high, next_ref[2 * pair], next_ref[2 * pair + 1]], axis=0)
            total = total + lax.dot_general(left, jnp.concatenate([high, low], axis=0), NT, preferred_element_type=F32)
        return total

    doubled = 2 * columns
    rows = doubled + 2 * bond
    total = lax.fori_loop(0, 2, products, jnp.zeros((rows, LANES), F32))
    row, lane = iota((rows, LANES), 0), iota((rows, LANES), 1)
    row_y = jnp.where(row < doubled, row // part % 2, (row >= doubled + bond).astype(jnp.int32))
    total = jnp.where(row_y == lane // part % 2, total, 0.0)
    lane, target = iota((LANES, doubled), 0), iota((LANES, doubled), 1)
    column = lane % doubled // own * part + lane % part
    pick = (column == target % columns) & ((target < columns) | (lane >= doubled))
    first = total.astype(BF16)
    thirds = jnp.concatenate([first, *halves(total - first.astype(F32))], axis=0)
    packed = jnp.dot(thirds, pick.astype(F32).astype(BF16), preferred_element_type=F32)
    packed = packed[:rows] + packed[rows:2 * rows] + packed[2 * rows:]
    squares = packed[:doubled].reshape(doubled // own, own, doubled)
    squares = squares + pltpu.roll(squares, part, 1)
    upper = iota((own, doubled), 0) < part
    squares = jnp.concatenate([jnp.where(upper, squares[2 * i], squares[2 * i + 1]) for i in range(columns // own)], axis=0)
    squeezes = packed[doubled:doubled + bond] + packed[doubled + bond:]
    padded = jnp.concatenate([squares, squeezes, jnp.zeros((LANES - columns - bond, doubled), F32)], axis=0)
    padded = jnp.concatenate([padded, jnp.zeros((LANES, LANES - doubled), F32)], axis=1)
    turned = padded.T
    gram = squares[:, :columns] + turned[columns:doubled, :columns]
    squeeze = turned[:columns, columns:columns + bond]
    flat = jnp.concatenate([v[8 * i:8 * i + 8] for v in (gram, squeeze) for i in range(columns // 8)], axis=1)
    blocks = fold(flat)
    for i, block in enumerate(blocks):
        sums_ref[i] = block


def fold(flat):
    blocks = []
    whole = flat.shape[1] // LANES * LANES
    for i in range(0, whole, LANES):
        blocks += [flat[:4, i:i + LANES], flat[4:, i:i + LANES]]
    if whole < flat.shape[1]:
        blocks.append(jnp.concatenate([flat[:4, whole:], flat[4:, whole:]], axis=1))
    return blocks


def unfold(blocks):
    flat = [jnp.concatenate(blocks[i:i + 2], axis=0) for i in range(0, len(blocks) - 1, 2)]
    if len(blocks) % 2:
        last = blocks[-1]
        flat.append(jnp.concatenate([last[:, :LANES // 2], last[:, LANES // 2:]], axis=0))
    return jnp.concatenate(flat, axis=1)


def sketch_products(far_own, far_other, near_high, near_low, nxt):
    columns, bond, quarter = near_high.shape
    width, own = nxt.shape[0], far_own.shape[3]
    shape = jax.ShapeDtypeStruct((width // 2, 2 * columns, quarter), BF16)
    blocks = columns * (columns + bond) // 512
    return pl.pallas_call(
        sketch_kernel,
        in_specs=[VMEM] * 5,
        out_specs=[VMEM] * 3,
        out_shape=[shape, shape, jax.ShapeDtypeStruct((blocks, 4, LANES), F32)],
        scratch_shapes=[
            pltpu.VMEM((width // 2, 2 * columns, quarter), F32),
            pltpu.VMEM((2 * columns // own, own * width, own // 2 * bond), BF16),
        ],
        cost_estimate=pl.CostEstimate(flops=2 * columns * bond * width * quarter * 24, bytes_accessed=8 * columns * width * quarter, transcendentals=0),
        compiler_params=params(16),
        name="sketch_products",
    )(far_own, far_other, near_high, near_low, nxt)


def pair_kernel(mine_ref, other_ref, out_ref):
    both = mine_ref[...] + other_ref[...]
    for i in range(out_ref.shape[0]):
        out_ref[i] = both


def pair_copies(mine, other, copies):
    return pl.pallas_call(
        pair_kernel,
        in_specs=[VMEM] * 2,
        out_specs=VMEM,
        out_shape=jax.ShapeDtypeStruct((copies,) + mine.shape, F32),
        compiler_params=params(8),
        name="pair_copies",
    )(mine, other)


def basis_kernel(count, sums_ref, high_ref, low_ref, basis_ref, squeezed_ref, square, out, out_sems):
    columns, width, quarter = basis_ref.shape
    bond = squeezed_ref.shape[1]

    def store(g, half):
        part = pl.ds(half * (columns // 2), columns // 2)
        target = basis_ref.at[part, pl.ds(pl.multiple_of(8 * g, 8), 8), :]
        return pltpu.make_async_copy(out.at[g, part], target, out_sems.at[half, g])

    summed = jnp.sum(sums_ref[...], axis=0)
    flat = unfold([summed[i] for i in range(summed.shape[0])])
    square[...] = jnp.zeros_like(square)
    for i in range(columns // 8):
        square[8 * i:8 * i + 8, :columns] = flat[:, i * columns:(i + 1) * columns] / count
        first = columns * (columns // 8) + i * bond
        square[8 * i:8 * i + 8, columns:columns + bond] = flat[:, first:first + bond]
    matrix = square[...]
    wide = 8 * columns
    within = iota((columns, wide), 1) % (2 * columns)
    unit = (within // 8 * 4 + within % 4 == iota((columns, wide), 0)).astype(F32)
    row = iota((columns, LANES), 0)
    roots = jnp.zeros((columns, LANES), F32)
    block = 16
    for first in range(0, columns, block):
        cols = [jnp.broadcast_to(matrix[:, first + j:first + j + 1], (columns, LANES)) for j in range(block)]
        for j in range(block):
            k = first + j
            pivot = cols[j][k:k + 1]
            factor = jnp.where(row > k, cols[j] * (1.0 / pivot), 0.0)
            for i in range(j + 1, block):
                cols[i] = cols[i] - factor * cols[i][k:k + 1]
            matrix = matrix - factor * matrix[k:k + 1]
            unit = unit - jnp.concatenate([factor] * (wide // LANES), axis=1) * unit[k:k + 1]
            roots = jnp.where(row == k, 1.0 / jnp.sqrt(pivot), roots)
    squeezed_ref[...] = (matrix * roots)[:, columns:columns + bond] / count ** 0.5
    inverse = unit * jnp.concatenate([roots] * (wide // LANES), axis=1)
    spread = jnp.broadcast_to(inverse[:, None, :], (columns, 8, wide)).reshape(wide, wide)
    lane = iota((wide, wide), 1)
    same = lane // (2 * columns) * 2 + lane // 4 % 2 == iota((wide, wide), 0) % 8
    left_high, left_low = halves(jnp.where(same, spread, 0.0))

    for g in range(width // 8):
        high = high_ref[4 * g:4 * g + 4].reshape(wide, quarter)
        low = low_ref[4 * g:4 * g + 4].reshape(wide, quarter)
        for half in range(2):
            rows = slice(half * (wide // 2), (half + 1) * (wide // 2))
            result = jnp.dot(left_high[rows], high, preferred_element_type=F32)
            result += jnp.dot(left_low[rows], high, preferred_element_type=F32)
            result += jnp.dot(left_high[rows], low, preferred_element_type=F32)
            out[g, half * (columns // 2):(half + 1) * (columns // 2)] = result.reshape(columns // 2, 8, quarter)
            store(g, half).start()
    for g in range(width // 8):
        for half in range(2):
            store(g, half).wait()


def basis_of(sums, high, low, bond, count):
    pairs, doubled, quarter = high.shape
    width, columns = 2 * pairs, doubled // 2
    return pl.pallas_call(
        functools.partial(basis_kernel, float(count)),
        in_specs=[VMEM] * 3,
        out_specs=[HBM, VMEM],
        out_shape=[jax.ShapeDtypeStruct((columns, width, quarter), F32), jax.ShapeDtypeStruct((columns, bond), F32)],
        scratch_shapes=[
            pltpu.VMEM((columns, LANES), F32),
            pltpu.VMEM((width // 8, columns, 8, quarter), F32),
            pltpu.SemaphoreType.DMA((2, width // 8)),
        ],
        cost_estimate=pl.CostEstimate(flops=2 * columns * columns * width * quarter * 24, bytes_accessed=4 * columns * width * quarter, transcendentals=0),
        compiler_params=params(16),
        name="basis_of",
    )(sums, high, low)


def per_device(factor_a, factor_b, next_factor, sketch_leg, sketch_rows):
    rows, cols = lax.axis_size("rows"), lax.axis_size("cols")
    devices = rows * cols
    local_rows, width, bond = factor_a.shape
    quarter = local_rows // cols
    count = local_rows * rows * width
    a = jnp.transpose(factor_a, (1, 2, 0))
    b = jnp.transpose(factor_b, (1, 2, 0)).reshape(width // 2, 2 * bond, local_rows)
    nxt = jnp.transpose(next_factor, (1, 2, 0))
    own = sketch_rows.shape[1]
    operands = [pltpu.with_memory_space_constraint(v, pltpu.HBM) for v in (sketch_rows.T, b, a)]
    partial, a_own = far_sum(*operands, quarter)
    each = -(-(width // 2) // rows)
    partial = jnp.pad(partial, ((0, each * rows - width // 2), (0, 0), (0, 0))).reshape(rows, each, own, LANES)
    parts = lax.all_to_all(partial, "rows", 0, 0)
    parities = [[i for i in range(devices) if i % 2 == parity] for parity in range(2)]
    pieces = lax.all_to_all(piece_copies(parts, devices // 2, bond), BOTH, 0, 0, axis_index_groups=parities)
    far_own = pieces.reshape(rows, cols // 2, each, own, LANES)
    swap = [(i, i ^ 1) for i in range(cols)]
    far_other = lax.ppermute(far_own, "cols", swap)
    near_high, near_low = near_sums(sketch_leg.T, a_own)
    high, low, sums = sketch_products(far_own, far_other, near_high, near_low, nxt)
    sums = pair_copies(sums, lax.ppermute(sums, "cols", swap), devices // 2)
    sums = lax.all_to_all(sums, BOTH, 0, 0, axis_index_groups=parities)
    basis, squeezed = basis_of(sums, high, low, bond, count)
    return jnp.transpose(basis, (0, 2, 1)), squeezed


def solution(mesh):
    return jax.shard_map(
        per_device,
        mesh=mesh,
        in_specs=(
            P("rows", None, None),
            P("rows", None, None),
            P(BOTH, None, None),
            P(),
            P("rows", "cols"),
        ),
        out_specs=(P(None, BOTH, None), P()),
        check_vma=False,
    )
```

```python
import functools

import jax
import jax.numpy as jnp
from jax import lax
from jax.experimental import pallas as pl
from jax.experimental.pallas import tpu as pltpu
from jax.sharding import PartitionSpec as P

BOTH = ("rows", "cols")
F32, BF16 = jnp.float32, jnp.bfloat16
LANES = 128
VMEM = pl.BlockSpec(memory_space=pltpu.VMEM)
HBM = pl.BlockSpec(memory_space=pltpu.HBM)
NT = (((1,), (1,)), ((), ()))


def iota(shape, axis):
    return lax.broadcasted_iota(jnp.int32, shape, axis)


def halves(value):
    high = value.astype(BF16)
    return high, (value - high.astype(F32)).astype(BF16)


def params(mib):
    return pltpu.CompilerParams(vmem_limit_bytes=mib << 20)


def far_kernel(rows_ref, b_ref, a_ref, out_ref, own_ref, rows_buf, buf, rows_sem, own_sem, sems):
    pairs, used, _ = b_ref.shape
    chunks = sems.shape[0]
    step = pairs // chunks
    quarter = own_ref.shape[2]
    start = pl.multiple_of(lax.axis_index("cols") * quarter, LANES)

    def fetch(c):
        part = pl.ds(c * step, step)
        return pltpu.make_async_copy(b_ref.at[part], buf.at[part], sems.at[c])

    rows_copy = pltpu.make_async_copy(rows_ref, rows_buf, rows_sem)
    rows_copy.start()
    ahead = 1
    for c in range(ahead):
        fetch(c).start()
    own_copy = pltpu.make_async_copy(a_ref.at[:, :, pl.ds(start, quarter)], own_ref, own_sem)
    own, lanes = out_ref.shape[1:]
    out_ref[:, :, used:] = jnp.zeros((pairs, own, lanes - used), F32)
    rows_copy.wait()
    for c in range(ahead, chunks):
        fetch(c).start()
    own_copy.start()
    for c in range(chunks):
        fetch(c).wait()
        for i in range(step):
            pair = c * step + i
            out_ref[pair, :, :used] = lax.dot_general(rows_buf[...], buf[pair], NT, preferred_element_type=F32)
    own_copy.wait()


def far_sum(rows_t, b_pairs, a_t, quarter):
    pairs, used, depth = b_pairs.shape
    chunks = pairs // 6
    own = rows_t.shape[0]
    return pl.pallas_call(
        far_kernel,
        in_specs=[HBM] * 3,
        out_specs=[VMEM] * 2,
        out_shape=[jax.ShapeDtypeStruct((pairs, own, LANES), F32), jax.ShapeDtypeStruct(a_t.shape[:2] + (quarter,), BF16)],
        scratch_shapes=[
            pltpu.VMEM(rows_t.shape, BF16),
            pltpu.VMEM((pairs, used, depth), BF16),
            pltpu.SemaphoreType.DMA,
            pltpu.SemaphoreType.DMA,
            pltpu.SemaphoreType.DMA((chunks,)),
        ],
        cost_estimate=pl.CostEstimate(flops=2 * own * pairs * used * depth, bytes_accessed=2 * pairs * used * depth, transcendentals=0),
        compiler_params=params(16),
        name="far_sum",
    )(rows_t, b_pairs, a_t)


def near_kernel(leg_ref, a_ref, high_ref, low_ref):
    columns, width = leg_ref.shape
    _, bond, quarter = high_ref.shape
    deep = 16
    wide = width * deep
    spread = (iota((width, wide), 1) // deep == iota((width, wide), 0)).astype(BF16)
    tiled = jnp.dot(leg_ref[...], spread, preferred_element_type=F32)
    tiled = jnp.broadcast_to(tiled[:, None, :], (columns, deep, wide)).reshape(columns * deep, wide)
    same = iota(tiled.shape, 1) % deep == iota(tiled.shape, 0) % deep
    weights = jnp.where(same, tiled, 0.0).astype(BF16)
    for first in range(0, bond, deep):
        part = a_ref[:, first:first + deep, :].reshape(wide, quarter)
        high, low = halves(jnp.dot(weights, part, preferred_element_type=F32))
        high_ref[:, first:first + deep, :] = high.reshape(columns, deep, quarter)
        low_ref[:, first:first + deep, :] = low.reshape(columns, deep, quarter)


def near_sums(leg_t, a_own):
    width, bond, quarter = a_own.shape
    columns = leg_t.shape[0]
    shape = jax.ShapeDtypeStruct((columns, bond, quarter), BF16)
    return pl.pallas_call(
        near_kernel,
        in_specs=[VMEM, VMEM],
        out_specs=[VMEM, VMEM],
        out_shape=[shape, shape],
        cost_estimate=pl.CostEstimate(flops=32 * columns * bond * width * quarter, bytes_accessed=2 * width * bond * quarter, transcendentals=0),
        compiler_params=params(16),
        name="near_sums",
    )(leg_t, a_own)


def piece_kernel(bond, parts_ref, out_ref):
    piece = jnp.sum(parts_ref[...], axis=0)
    half = piece.shape[1] // 2
    crossed = pltpu.roll(piece, half, 1)
    upper = iota(piece.shape, 1) < half
    left = iota(piece.shape, 2) < bond
    crossed = jnp.where(upper, pltpu.roll(crossed, bond, 2), pltpu.roll(crossed, LANES - bond, 2))
    piece = jnp.where(upper == left, piece, crossed)
    for i in range(out_ref.shape[0]):
        out_ref[i] = piece


def piece_copies(parts, copies, bond):
    return pl.pallas_call(
        functools.partial(piece_kernel, bond),
        in_specs=[VMEM],
        out_specs=VMEM,
        out_shape=jax.ShapeDtypeStruct((copies,) + parts.shape[1:], F32),
        compiler_params=params(8),
        name="piece_copies",
    )(parts)


def sketch_kernel(own_ref, other_ref, near_high_ref, near_low_ref, next_ref, high_ref, low_ref, sums_ref, sketch, wide_ref):
    groups, own = own_ref.shape[1], own_ref.shape[3]
    columns, bond, quarter = near_high_ref.shape
    pairs = sketch.shape[0]
    part = own // 2
    wide = part * bond
    parity = lax.axis_index("cols") % 2
    lane = iota((LANES, wide), 1) % bond
    keep = [(iota((LANES, wide), 0) == lane + half * bond).astype(BF16) for half in range(2)]
    same = iota((pairs * own, wide), 1) // bond == iota((pairs * own, wide), 0) % part

    def widen(far_ref, odd, g):
        far = halves(far_ref[:, g].reshape(-1, LANES)[:pairs * own])
        for half in range(2):
            block = 2 * (2 * g + odd) + half
            for i, piece in enumerate(far):
                value = jnp.dot(piece, keep[half], preferred_element_type=F32)
                wide_ref[block, pl.ds(i * pairs * own, pairs * own), :] = jnp.where(same, value, 0.0).astype(BF16)

    for g in range(groups):
        widen(own_ref, parity, g)
        widen(other_ref, 1 - parity, g)
    for block in range(columns // part):
        near_high = near_high_ref[block * part:(block + 1) * part].reshape(wide, quarter)
        near_low = near_low_ref[block * part:(block + 1) * part].reshape(wide, quarter)
        both = jnp.dot(wide_ref[block], near_high, preferred_element_type=F32)
        cross = jnp.dot(wide_ref[block, :pairs * own, :], near_low, preferred_element_type=F32)
        result = both[:pairs * own] + both[pairs * own:] + cross
        sketch[:, block * own:(block + 1) * own, :] = result.reshape(pairs, own, quarter)

    def products(i, total):
        for step in range(pairs // 2):
            pair = pairs // 2 * i + step
            high, low = halves(sketch[pair])
            high_ref[pair] = high
            low_ref[pair] = low
            left = jnp.concatenate([high, next_ref[2 * pair], next_ref[2 * pair + 1]], axis=0)
            total = total + lax.dot_general(left, jnp.concatenate([high, low], axis=0), NT, preferred_element_type=F32)
        return total

    doubled = 2 * columns
    rows = doubled + 2 * bond
    total = lax.fori_loop(0, 2, products, jnp.zeros((rows, LANES), F32))
    row, lane = iota((rows, LANES), 0), iota((rows, LANES), 1)
    row_y = jnp.where(row < doubled, row // part % 2, (row >= doubled + bond).astype(jnp.int32))
    total = jnp.where(row_y == lane // part % 2, total, 0.0)
    lane, target = iota((LANES, doubled), 0), iota((LANES, doubled), 1)
    column = lane % doubled // own * part + lane % part
    pick = (column == target % columns) & ((target < columns) | (lane >= doubled))
    packed = jnp.dot(total, pick.astype(F32), preferred_element_type=F32, precision=lax.Precision.HIGHEST)
    squares = packed[:doubled].reshape(doubled // own, own, doubled)
    squares = squares + pltpu.roll(squares, part, 1)
    upper = iota((own, doubled), 0) < part
    squares = jnp.concatenate([jnp.where(upper, squares[2 * i], squares[2 * i + 1]) for i in range(columns // own)], axis=0)
    squeezes = packed[doubled:doubled + bond] + packed[doubled + bond:]
    padded = jnp.concatenate([squares, squeezes, jnp.zeros((LANES - columns - bond, doubled), F32)], axis=0)
    padded = jnp.concatenate([padded, jnp.zeros((LANES, LANES - doubled), F32)], axis=1)
    turned = padded.T
    gram = squares[:, :columns] + turned[columns:doubled, :columns]
    squeeze = turned[:columns, columns:columns + bond]
    flat = jnp.concatenate([v[8 * i:8 * i + 8] for v in (gram, squeeze) for i in range(columns // 8)], axis=1)
    blocks = fold(flat)
    for i, block in enumerate(blocks):
        sums_ref[i] = block


def fold(flat):
    blocks = []
    whole = flat.shape[1] // LANES * LANES
    for i in range(0, whole, LANES):
        blocks += [flat[:4, i:i + LANES], flat[4:, i:i + LANES]]
    if whole < flat.shape[1]:
        blocks.append(jnp.concatenate([flat[:4, whole:], flat[4:, whole:]], axis=1))
    return blocks


def unfold(blocks):
    flat = [jnp.concatenate(blocks[i:i + 2], axis=0) for i in range(0, len(blocks) - 1, 2)]
    if len(blocks) % 2:
        last = blocks[-1]
        flat.append(jnp.concatenate([last[:, :LANES // 2], last[:, LANES // 2:]], axis=0))
    return jnp.concatenate(flat, axis=1)


def sketch_products(far_own, far_other, near_high, near_low, nxt):
    columns, bond, quarter = near_high.shape
    width, own = nxt.shape[0], far_own.shape[3]
    shape = jax.ShapeDtypeStruct((width // 2, 2 * columns, quarter), BF16)
    blocks = columns * (columns + bond) // 512
    return pl.pallas_call(
        sketch_kernel,
        in_specs=[VMEM] * 5,
        out_specs=[VMEM] * 3,
        out_shape=[shape, shape, jax.ShapeDtypeStruct((blocks, 4, LANES), F32)],
        scratch_shapes=[
            pltpu.VMEM((width // 2, 2 * columns, quarter), F32),
            pltpu.VMEM((2 * columns // own, own * width, own // 2 * bond), BF16),
        ],
        cost_estimate=pl.CostEstimate(flops=2 * columns * bond * width * quarter * 24, bytes_accessed=8 * columns * width * quarter, transcendentals=0),
        compiler_params=params(16),
        name="sketch_products",
    )(far_own, far_other, near_high, near_low, nxt)


def pair_kernel(mine_ref, other_ref, out_ref):
    both = mine_ref[...] + other_ref[...]
    for i in range(out_ref.shape[0]):
        out_ref[i] = both


def pair_copies(mine, other, copies):
    return pl.pallas_call(
        pair_kernel,
        in_specs=[VMEM] * 2,
        out_specs=VMEM,
        out_shape=jax.ShapeDtypeStruct((copies,) + mine.shape, F32),
        compiler_params=params(8),
        name="pair_copies",
    )(mine, other)


def basis_kernel(count, sums_ref, high_ref, low_ref, basis_ref, squeezed_ref, square, out, out_sems):
    columns, width, quarter = basis_ref.shape
    bond = squeezed_ref.shape[1]

    def store(g):
        return pltpu.make_async_copy(out.at[g], basis_ref.at[:, pl.ds(pl.multiple_of(8 * g, 8), 8), :], out_sems.at[g])

    summed = jnp.sum(sums_ref[...], axis=0)
    flat = unfold([summed[i] for i in range(summed.shape[0])])
    square[...] = jnp.zeros_like(square)
    for i in range(columns // 8):
        square[8 * i:8 * i + 8, :columns] = flat[:, i * columns:(i + 1) * columns] / count
        first = columns * (columns // 8) + i * bond
        square[8 * i:8 * i + 8, columns:columns + bond] = flat[:, first:first + bond]
    matrix = square[...]
    wide = 8 * columns
    within = iota((columns, wide), 1) % (2 * columns)
    unit = (within // 8 * 4 + within % 4 == iota((columns, wide), 0)).astype(F32)
    row = iota((columns, LANES), 0)
    roots = jnp.zeros((columns, LANES), F32)
    block = 16
    for first in range(0, columns, block):
        cols = [jnp.broadcast_to(matrix[:, first + j:first + j + 1], (columns, LANES)) for j in range(block)]
        for j in range(block):
            k = first + j
            pivot = cols[j][k:k + 1]
            factor = jnp.where(row > k, cols[j] * (1.0 / pivot), 0.0)
            for i in range(j + 1, block):
                cols[i] = cols[i] - factor * cols[i][k:k + 1]
            matrix = matrix - factor * matrix[k:k + 1]
            unit = unit - jnp.concatenate([factor] * (wide // LANES), axis=1) * unit[k:k + 1]
            roots = jnp.where(row == k, 1.0 / jnp.sqrt(pivot), roots)
    squeezed_ref[...] = (matrix * roots)[:, columns:columns + bond] / count ** 0.5
    inverse = unit * jnp.concatenate([roots] * (wide // LANES), axis=1)
    spread = jnp.broadcast_to(inverse[:, None, :], (columns, 8, wide)).reshape(wide, wide)
    lane = iota((wide, wide), 1)
    same = lane // (2 * columns) * 2 + lane // 4 % 2 == iota((wide, wide), 0) % 8
    left_high, left_low = halves(jnp.where(same, spread, 0.0))

    def group(g, carry):
        high = high_ref[pl.ds(4 * g, 4)].reshape(wide, quarter)
        low = low_ref[pl.ds(4 * g, 4)].reshape(wide, quarter)
        result = jnp.dot(left_high, high, preferred_element_type=F32)
        result += jnp.dot(left_low, high, preferred_element_type=F32)
        result += jnp.dot(left_high, low, preferred_element_type=F32)
        out[g] = result.reshape(columns, 8, quarter)
        store(g).start()
        return carry

    lax.fori_loop(0, width // 8, group, 0, unroll=True)
    lax.fori_loop(0, width // 8, lambda g, carry: (store(g).wait(), carry)[1], 0)


def basis_of(sums, high, low, bond, count):
    pairs, doubled, quarter = high.shape
    width, columns = 2 * pairs, doubled // 2
    return pl.pallas_call(
        functools.partial(basis_kernel, float(count)),
        in_specs=[VMEM] * 3,
        out_specs=[HBM, VMEM],
        out_shape=[jax.ShapeDtypeStruct((columns, width, quarter), F32), jax.ShapeDtypeStruct((columns, bond), F32)],
        scratch_shapes=[
            pltpu.VMEM((columns, LANES), F32),
            pltpu.VMEM((width // 8, columns, 8, quarter), F32),
            pltpu.SemaphoreType.DMA((width // 8,)),
        ],
        cost_estimate=pl.CostEstimate(flops=2 * columns * columns * width * quarter * 24, bytes_accessed=4 * columns * width * quarter, transcendentals=0),
        compiler_params=params(16),
        name="basis_of",
    )(sums, high, low)


def per_device(factor_a, factor_b, next_factor, sketch_leg, sketch_rows):
    rows, cols = lax.axis_size("rows"), lax.axis_size("cols")
    devices = rows * cols
    local_rows, width, bond = factor_a.shape
    quarter = local_rows // cols
    count = local_rows * rows * width
    a = jnp.transpose(factor_a, (1, 2, 0))
    b = jnp.transpose(factor_b, (1, 2, 0)).reshape(width // 2, 2 * bond, local_rows)
    nxt = jnp.transpose(next_factor, (1, 2, 0))
    own = sketch_rows.shape[1]
    operands = [pltpu.with_memory_space_constraint(v, pltpu.HBM) for v in (sketch_rows.T, b, a)]
    partial, a_own = far_sum(*operands, quarter)
    each = -(-(width // 2) // rows)
    partial = jnp.pad(partial, ((0, each * rows - width // 2), (0, 0), (0, 0))).reshape(rows, each, own, LANES)
    parts = lax.all_to_all(partial, "rows", 0, 0)
    parities = [[i for i in range(devices) if i % 2 == parity] for parity in range(2)]
    pieces = lax.all_to_all(piece_copies(parts, devices // 2, bond), BOTH, 0, 0, axis_index_groups=parities)
    far_own = pieces.reshape(rows, cols // 2, each, own, LANES)
    swap = [(i, i ^ 1) for i in range(cols)]
    far_other = lax.ppermute(far_own, "cols", swap)
    near_high, near_low = near_sums(sketch_leg.T, a_own)
    high, low, sums = sketch_products(far_own, far_other, near_high, near_low, nxt)
    sums = pair_copies(sums, lax.ppermute(sums, "cols", swap), devices // 2)
    sums = lax.all_to_all(sums, BOTH, 0, 0, axis_index_groups=parities)
    basis, squeezed = basis_of(sums, high, low, bond, count)
    return jnp.transpose(basis, (0, 2, 1)), squeezed


def solution(mesh):
    return jax.shard_map(
        per_device,
        mesh=mesh,
        in_specs=(
            P("rows", None, None),
            P("rows", None, None),
            P(BOTH, None, None),
            P(),
            P("rows", "cols"),
        ),
        out_specs=(P(None, BOTH, None), P()),
        check_vma=False,
    )
```
